8 devices in a mesh: dp: 2 (over y, z), tp: 4 (over x, core).
Axes of the slice: x: 2, y: 2, z: 1, core: 2. Of those that a mesh axis runs over, the one named last changes fastest.
Arguments:
- x: bfloat16 [2048, 4096], P(('dp', 'tp')), parts along dimension 0
- gain_a: bfloat16 [4096], replicated
- wq: bfloat16 [4096, 4096], P(None, 'tp')
- wk: bfloat16 [4096, 1024], P(None, 'tp')
- wv: bfloat16 [4096, 1024], P(None, 'tp')
- wo: bfloat16 [4096, 4096], P('tp')
- gain_m: bfloat16 [4096], replicated
- w_gate: bfloat16 [4096, 12800], P(None, 'tp')
- w_up: bfloat16 [4096, 12800], P(None, 'tp')
- w_down: bfloat16 [12800, 4096], P('tp')
Outputs:
- output: bfloat16 [2048, 4096], P(('dp', 'tp')), parts along dimension 0
There are 2 independent parts. The reference program is written for one: setup_inputs(seed, part) draws one part's arguments, and reference() takes and returns one part's arrays. A program takes and returns all parts, laid end to end along the dimension named above; an argument that names none is the same for every part.
All inputs are finite; a program needn't handle non-finite values.
Results may differ from the reference program's by a relative error of at most 0.017.
Values are sent between devices in bfloat16 or wider.
A program may use at most 2 GiB of HBM per device.

```python
import jax
import jax.numpy as jnp
from jax import lax

ROWS = 1024
D = 4096
HEADS = 32
KV_HEADS = 8
HEAD = 128
FF = 12800
THETA = 10000


def setup_inputs(seed: int = 0, part: int = 0) -> dict:
    kx, kn, kq, kk, kv, ko, km, kg, ku, kd = jax.random.split(jax.random.key(seed), 10)

    def weights(key, rows, columns):
        return jax.random.normal(key, (rows, columns), jnp.float32) * rows**-0.5

    drawn = {
        "x": jax.random.normal(jax.random.fold_in(kx, part), (ROWS, D), jnp.float32),
        "gain_a": 1 + 0.1 * jax.random.normal(kn, (D,), jnp.float32),
        "wq": 2 * weights(kq, D, HEADS * HEAD),
        "wk": 2 * weights(kk, D, KV_HEADS * HEAD),
        "wv": 4 * weights(kv, D, KV_HEADS * HEAD),
        "wo": weights(ko, HEADS * HEAD, D),
        "gain_m": 1 + 0.1 * jax.random.normal(km, (D,), jnp.float32),
        "w_gate": weights(kg, D, FF),
        "w_up": weights(ku, D, FF),
        "w_down": 2 * weights(kd, FF, D),
    }
    return {k: v.astype(jnp.bfloat16) for k, v in drawn.items()}


def normed(x, gain):
    wide = x.astype(jnp.float32)
    scale = lax.rsqrt(jnp.mean(wide * wide, -1, keepdims=True) + 1e-6)
    return (wide * scale * gain.astype(jnp.float32)).astype(jnp.bfloat16)


def turned(t, place, theta):
    half = t.shape[-1] // 2
    angle = place.astype(jnp.float32)[:, None] * theta ** (-jnp.arange(half, dtype=jnp.float32) / half)
    cos, sin = jnp.cos(angle)[:, None], jnp.sin(angle)[:, None]
    a, b = t[..., :half].astype(jnp.float32), t[..., half:].astype(jnp.float32)
    return jnp.concatenate([a * cos - b * sin, b * cos + a * sin], -1).astype(jnp.bfloat16)


def matmul(a, w):
    return jnp.dot(a, w, preferred_element_type=jnp.float32).astype(jnp.bfloat16)


def einsum(form, a, b):
    return jnp.einsum(form, a.astype(jnp.float32), b.astype(jnp.float32))


def attention(q, k, v):
    scores = einsum("tgsd,ugd->gstu", q, k) * q.shape[-1] ** -0.5
    token = jnp.arange(q.shape[0])
    scores = jnp.where(token[:, None] >= token, scores, -jnp.inf)
    weights = jax.nn.softmax(scores, -1).astype(jnp.bfloat16)
    return einsum("gstu,ugd->tgsd", weights, v).astype(jnp.bfloat16)


def reference(x, gain_a, wq, wk, wv, wo, gain_m, w_gate, w_up, w_down):
    a, place = normed(x, gain_a), jnp.arange(ROWS)
    q = turned(matmul(a, wq).reshape(ROWS, HEADS, HEAD), place, THETA).reshape(ROWS, KV_HEADS, -1, HEAD)
    k = turned(matmul(a, wk).reshape(ROWS, KV_HEADS, HEAD), place, THETA)
    v = matmul(a, wv).reshape(ROWS, KV_HEADS, HEAD)
    seen = attention(q, k, v).reshape(ROWS, HEADS * HEAD)
    h = (x.astype(jnp.float32) + jnp.dot(seen, wo, preferred_element_type=jnp.float32)).astype(jnp.bfloat16)
    b = normed(h, gain_m)
    gate = jnp.dot(b, w_gate, preferred_element_type=jnp.float32)
    up = jnp.dot(b, w_up, preferred_element_type=jnp.float32)
    hidden = (jax.nn.silu(gate) * up).astype(jnp.bfloat16)
    return (h.astype(jnp.float32) + jnp.dot(hidden, w_down, preferred_element_type=jnp.float32)).astype(jnp.bfloat16)
```

```python
import functools

import jax
import jax.numpy as jnp
import numpy as np
from jax import lax
from jax.experimental import pallas as pl
from jax.experimental.pallas import tpu as pltpu
from jax.sharding import PartitionSpec as P

MESH = pl.DeviceIdType.MESH
BF, F32 = jnp.bfloat16, jnp.float32
HEAD = 128
THETA = 10000
NEG = -1e30
HIDDEN = 2 * NEG
E = HEAD**-0.5 * 1.4426950408889634
HALF = 128
WIDE = 1024
VMEM_LIMIT = 67043328


def dot(a, b):
    return jnp.dot(a, b, preferred_element_type=F32)


class Place:
    def __init__(self):
        tp, dp = lax.axis_index("tp"), lax.axis_index("dp")
        self.c, self.x = lax.rem(tp, 2), lax.div(tp, 2)
        self.partner = (dp, self.x * 2 + (1 - self.c))
        self.across = (dp, (1 - self.x) * 2 + self.c)

    def greet(self):
        barrier = pltpu.get_barrier_semaphore()
        for who in (self.partner, self.across):
            pl.semaphore_signal(barrier, inc=1, device_id=who, device_id_type=MESH)
        pl.semaphore_wait(barrier, 2)


def remote(src, dst, sems, at, who):
    return pltpu.make_async_remote_copy(
        src_ref=src, dst_ref=dst, send_sem=sems.at[(0, *at)], recv_sem=sems.at[(1, *at)], device_id=who, device_id_type=MESH
    )


def norm_into(src, dst, gain, first):
    @pl.loop(0, HALF // 32)
    def _(i):
        rows = pl.ds(first + i * 32, 32)
        wide = src[rows, :].astype(F32)
        scale = lax.rsqrt(jnp.mean(wide * wide, -1, keepdims=True) + 1e-6)
        dst[rows, :] = (wide * scale * gain[...].astype(F32)).astype(BF)


class Gather:
    def __init__(self, a, own, cross, hand, place):
        rows = [pl.ds(k * HALF, HALF) for k in range(2)]
        self.own = [remote(a.at[0, r], a.at[1, r], own, (k,), place.partner) for k, r in enumerate(rows)]
        self.cross = [remote(a.at[0, r], a.at[2 + k, rows[0]], cross, (k,), place.across) for k, r in enumerate(rows)]
        self.hand = [remote(a.at[2 + k, rows[0]], a.at[2 + k, rows[1]], hand, (k,), place.partner) for k in range(2)]

    def start(self, k):
        self.cross[k].start()
        self.own[k].start()

    def drain(self):
        for c in (*self.own, *self.cross, *self.hand):
            c.wait_send()


def attention_half(x_hbm, gain, tab_hbm, wq, wk, wv, wo, h_hbm, xb, a, w3, wov, tab, tq, qb, kb, vt, seen, top, mix, gap, acc, ds, dr, xs,
                   xr, hb, load_sem, w_sem, wo_sem, own_sem, cross_sem, hand_sem, pair_sem, sum_sem, out_sem):
    place = Place()
    c, x = place.c, place.x
    load = pltpu.make_async_copy(x_hbm, xb, load_sem.at[0])
    load.start()
    load_tab = pltpu.make_async_copy(tab_hbm, tab, load_sem.at[1])
    load_tab.start()
    loads = [
        pltpu.make_async_copy(wq.at[:, 0:512], w3.at[0], w_sem.at[0]),
        pltpu.make_async_copy(wq.at[:, 512:1024], w3.at[1], w_sem.at[1]),
        pltpu.make_async_copy(wk, w3.at[2, :, 0:256], w_sem.at[2]),
        pltpu.make_async_copy(wv, w3.at[2, :, 256:512], w_sem.at[3]),
    ]
    loads_o = [pltpu.make_async_copy(wo.at[:, t * WIDE : (t + 1) * WIDE], wov.at[t], wo_sem.at[t]) for t in range(4)]
    gather = Gather(a, own_sem, cross_sem, hand_sem, place)
    place.greet()
    load.wait()
    for k in range(2):
        norm_into(xb, a.at[0], gain, k * HALF)
        gather.start(k)
        if k == 0:
            for w in loads:
                w.start()
    for w in loads_o:
        w.start()
    kb[...] = jnp.zeros_like(kb)
    vt[...] = jnp.zeros_like(vt)
    vt[:, HEAD:, :] = jnp.ones((2, 16, 1024), BF)
    gap[...] = lax.rem(lax.broadcasted_iota(jnp.int32, gap.shape, 1), HALF) - lax.broadcasted_iota(jnp.int32, gap.shape, 0)
    load_tab.wait()
    for w in loads:
        w.wait()

    def to_pair(s, k, t):
        return remote(ds.at[s, k, t], dr.at[s, k, t], pair_sem, (s, k, t), place.partner)

    def to_across(k, t):
        return remote(xs.at[k, t], xr.at[k, t], sum_sem, (k, t), place.across)

    def project(u):
        far = lax.div(u, 2)
        core = c + u * (1 - 2 * c)
        b0 = (1 - far) * (x * 4 + core * 2) + far * ((1 - x) * 4 + c * 2 + u - 2)
        b1 = (1 - far) * (x * 4 + core * 2 + 1) + far * ((1 - x) * 4 + (1 - c) * 2 + u - 2)

        @pl.loop(0, 3)
        def _(j):
            tq[...] = dot(a[u], w3[j]).astype(BF)
            for half, b in enumerate((b0, b1)):
                rows = pl.ds(pl.multiple_of(b * HALF, HALF), HALF)

                def part(n, half=half):
                    return tq[half * HALF : (half + 1) * HALF, n * HEAD : (n + 1) * HEAD]

                def turned(n, b=b, part=part):
                    t = part(n).astype(F32)
                    return (t * tab[0, b] + pltpu.roll(t, HEAD // 2, 1) * tab[1, b]).astype(BF)

                @pl.when(j < 2)
                def _():
                    for n in range(4):
                        qb[b, j * 4 + n] = turned(n)

                @pl.when(j == 2)
                def _():
                    for n in range(2):
                        kb[n, rows, :] = turned(n)
                        vt[n, :HEAD, rows] = part(2 + n).T

    def block(i):
        s, o, k = lax.div(i, 4), lax.div(lax.rem(i, 4), 2), lax.rem(i, 2)
        b = ((1 - s) * (1 - x) + s * x) * 4 + lax.rem(i, 4)
        top[...] = jnp.full_like(top, NEG)
        mix[...] = jnp.zeros_like(mix)

        @pl.loop(0, lax.div(b, 2) + 1)
        def _(j):
            keys = pl.ds(pl.multiple_of(j * 256, 256), 256)
            ok = gap[...] >= j * 256 - b * HALF
            scores = [
                lax.dot_general(kb[g, keys, :], qb[b, 4 * g : 4 * g + 4].reshape(512, HEAD), (((1,), (1,)), ((), ())), preferred_element_type=F32)
                for g in range(2)
            ]
            weights, keeps = [], []
            for g in range(2):
                sc = jnp.where(ok, scores[g], HIDDEN)
                old = top[g : g + 1, :]
                new = jnp.maximum(old, sc.max(axis=0, keepdims=True))
                top[g : g + 1, :] = new
                weights.append(jnp.exp2((sc - new) * E).astype(BF))
                keeps.append(jnp.exp2((old - new) * E))
            for g in range(2):
                mix[g] = mix[g] * keeps[g] + dot(vt[g, :, keys], weights[g])

        for g in range(2):
            out = mix[g, :HEAD, :] * (1 / mix[g, HEAD : HEAD + 1, :])
            for n in range(4):
                seen[:, (4 * g + n) * HEAD : (4 * g + n + 1) * HEAD] = out[:, n * HEAD : (n + 1) * HEAD].T.astype(BF)

        @pl.loop(0, 4)
        def _(t):
            r = dot(seen[...], wov[t])

            @pl.when(o == c)
            def _():
                acc[s, k, t] = r

            @pl.when(o != c)
            def _():
                ds[s, k, t] = r.astype(BF)
                to_pair(s, k, t).start()

    def combine(k):
        @pl.loop(0, 4)
        def _(t):
            to_pair(0, k, t).wait_recv()
            xs[k, t] = (acc[0, k, t] + dr[0, k, t].astype(F32)).astype(BF)
            to_across(k, t).start()

    @pl.loop(0, 4)
    def _(u):
        @pl.when(u == 1)
        def _():
            for w in gather.own:
                w.wait_recv()

        @pl.when(u == 2)
        def _():
            gather.cross[0].wait_recv()
            gather.hand[0].start()
            gather.hand[0].wait_recv()

        @pl.when(u == 3)
        def _():
            gather.cross[1].wait_recv()
            gather.hand[1].start()

            @pl.when(c == 0)
            def _():
                combine(0)

            gather.hand[1].wait_recv()

        project(u)

        @pl.when(u == 2)
        def _():
            for w in loads_o:
                w.wait()
            block(0)

    @pl.loop(1, 8)
    def _(i):
        block(i)

        @pl.when((i < 4) & (lax.div(i, 2) == c))
        def _():
            combine(lax.rem(i, 2))

    def out(k, t):
        rows, cols = pl.ds(pl.multiple_of(k * HALF, HALF), HALF), pl.ds(pl.multiple_of(t * WIDE, WIDE), WIDE)
        return pltpu.make_async_copy(hb.at[k, t], h_hbm.at[rows, cols], out_sem.at[k, t])

    @pl.loop(0, 8)
    def _(i):
        k, t = lax.div(i, 4), lax.rem(i, 4)
        to_pair(1, k, t).wait_recv()
        to_across(k, t).wait_recv()
        rows, cols = pl.ds(pl.multiple_of(k * HALF, HALF), HALF), pl.ds(pl.multiple_of(t * WIDE, WIDE), WIDE)
        term = acc[1, k, t] + dr[1, k, t].astype(F32) + xr[k, t].astype(F32)
        hb[k, t] = (xb[rows, cols].astype(F32) + term).astype(BF)
        out(k, t).start()

    @pl.loop(0, 8)
    def _(i):
        k, t = lax.div(i, 4), lax.rem(i, 4)
        out(k, t).wait()
        to_across(k, t).wait_send()
        to_pair(0, k, t).wait_send()
        to_pair(1, k, t).wait_send()

    gather.drain()


PART = 256
GU_SLOTS, D_SLOTS = 3, 2


def mlp_half(h_hbm, gain, wg, wu, wd, y_hbm, h, a, hid, hidf, gu, dn, accf, fs, fr, xs, xr, acco, os_, or_, yb, load_sem, gu_sem, d_sem,
             own_sem, cross_sem, hand_sem, fpair_sem, sum_sem, opair_sem, out_sem):
    place = Place()
    units = wg.shape[1]
    full = units // PART
    tiles = full + 1
    load = pltpu.make_async_copy(h_hbm, h, load_sem.at[0])
    load.start()

    def gu_tile(j, slot):
        cols = pl.ds(pl.multiple_of(j * PART, PART), PART)
        return [
            pltpu.make_async_copy(wg.at[:, cols], gu.at[slot, :, 0:PART], gu_sem.at[slot, 0]),
            pltpu.make_async_copy(wu.at[:, cols], gu.at[slot, :, PART : 2 * PART], gu_sem.at[slot, 1]),
        ]

    def gu_last(slot):
        cols, half = pl.ds(full * PART, PART // 2), PART // 2
        return [
            pltpu.make_async_copy(wg.at[:, cols], gu.at[slot, :, 0:half], gu_sem.at[slot, 0]),
            pltpu.make_async_copy(wu.at[:, cols], gu.at[slot, :, half:PART], gu_sem.at[slot, 1]),
        ]

    def d_tile(t):
        slot = lax.rem(t, D_SLOTS)
        cols = pl.ds(pl.multiple_of(t * WIDE, WIDE), WIDE)
        return pltpu.make_async_copy(wd.at[:, cols], dn.at[slot], d_sem.at[slot])

    gather = Gather(a, own_sem, cross_sem, hand_sem, place)
    place.greet()
    load.wait()
    for k in range(2):
        norm_into(h, a.at[0], gain, k * HALF)
        gather.start(k)
        if k == 0:
            for j in range(GU_SLOTS):
                for w in gu_tile(j, j):
                    w.start()
    for t in range(D_SLOTS):
        d_tile(t).start()

    def hidden(p, lhs, out, also):
        @pl.loop(0, full)
        def _(j):
            slot = lax.rem(p + j, GU_SLOTS)
            for w in gu_tile(j, slot):
                w.wait()
            r = dot(lhs[...], gu[slot])
            out[:, pl.ds(pl.multiple_of(j * PART, PART), PART)] = (jax.nn.silu(r[:, :PART]) * r[:, PART:]).astype(BF)
            later = j + GU_SLOTS

            @pl.when(later < full)
            def _():
                for w in gu_tile(later, slot):
                    w.start()

            @pl.when(later == full)
            def _():
                for w in gu_last(slot):
                    w.start()

            @pl.when((later > full) & (p < 2))
            def _():
                for w in gu_tile(later - tiles, slot):
                    w.start()

            also(j)

        slot = lax.rem(p + full, GU_SLOTS)
        for w in gu_last(slot):
            w.wait()
        r = dot(lhs[...], gu[slot, :, 0:PART])
        out[:, full * PART :] = (jax.nn.silu(r[:, : PART // 2]) * r[:, PART // 2 :]).astype(BF)

        @pl.when(p < 2)
        def _():
            for w in gu_tile(GU_SLOTS - 1, slot):
                w.start()

    def fpair(k, t):
        return remote(fs.at[k, t], fr.at[k, t], fpair_sem, (k, t), place.partner)

    def to_across(k, t):
        return remote(xs.at[k, t], xr.at[k, t], sum_sem, (k, t), place.across)

    def combine(k, t):
        fpair(k, t).wait_recv()
        xs[k, t] = (accf[t] + fr[k, t].astype(F32)).astype(BF)
        to_across(k, t).start()

    def first_also(j):
        @pl.when(j == full - 2)
        def _():
            gather.cross[0].wait_recv()
            gather.hand[0].start()

    for w in gather.own:
        w.wait_recv()
    hidden(0, a.at[0:2].reshape(4 * HALF, a.shape[2]), hid, first_also)

    @pl.loop(0, 2)
    def _(k):
        @pl.when(k == 0)
        def _():
            gather.hand[0].wait_recv()

        @pl.when(k == 1)
        def _():
            gather.hand[1].wait_recv()

        def also(j):
            @pl.when((j == 1) & (k == 1))
            def _():
                combine(0, 3)

        hidden(1 + k, a.at[2 + k], hidf, also)

        @pl.when(k == 0)
        def _():
            gather.cross[1].wait_recv()
            gather.hand[1].start()

        @pl.loop(0, 4)
        def _(t):
            d_tile(t).wait()
            r = dot(hidf[...], dn[lax.rem(t, D_SLOTS)])
            d_tile(lax.rem(t + D_SLOTS, 4)).start()
            accf[t] = r[:HALF]
            fs[k, t] = r[HALF:].astype(BF)
            fpair(k, t).start()

            @pl.when(t > 0)
            def _():
                combine(k, t - 1)

    def opair(t):
        return remote(os_.at[t], or_.at[t], opair_sem, (t,), place.partner)

    def out(t):
        return pltpu.make_async_copy(yb.at[t], y_hbm.at[:, pl.ds(pl.multiple_of(t * WIDE, WIDE), WIDE)], out_sem.at[t])

    def finish(t):
        opair(t).wait_recv()
        cols = pl.ds(pl.multiple_of(t * WIDE, WIDE), WIDE)
        for k in range(2):
            to_across(k, t).wait_recv()
            rows = slice(k * HALF, (k + 1) * HALF)
            term = acco[t, rows] + or_[t, rows].astype(F32) + xr[k, t].astype(F32)
            yb[t, rows] = (h[rows, cols].astype(F32) + term).astype(BF)
        out(t).start()

    @pl.loop(0, 4)
    def _(t):
        d_tile(t).wait()
        r = dot(hid[...], dn[lax.rem(t, D_SLOTS)])

        @pl.when(t < 2)
        def _():
            d_tile(t + D_SLOTS).start()

        acco[t] = r[: 2 * HALF]
        os_[t] = r[2 * HALF :].astype(BF)
        opair(t).start()

        @pl.when(t == 0)
        def _():
            combine(1, 3)

        @pl.when(t > 0)
        def _():
            finish(t - 1)

    finish(3)

    @pl.loop(0, 4)
    def _(t):
        out(t).wait()
        opair(t).wait_send()
        for k in range(2):
            to_across(k, t).wait_send()
            fpair(k, t).wait_send()

    gather.drain()


def call(body, name, ident, args, spaces, scratch, shape, flops, moved):
    specs = [pl.BlockSpec(memory_space=s) for s in spaces]
    return pl.pallas_call(
        body,
        out_shape=jax.ShapeDtypeStruct(shape, BF),
        in_specs=specs,
        out_specs=pl.BlockSpec(memory_space=pl.ANY),
        scratch_shapes=scratch,
        compiler_params=pltpu.CompilerParams(collective_id=ident, has_side_effects=True, vmem_limit_bytes=VMEM_LIMIT),
        cost_estimate=pl.CostEstimate(flops=flops, bytes_accessed=moved, transcendentals=0),
        name=name,
    )(*args)


def turns(rows):
    half = HEAD // 2
    rate = (float(THETA) ** (-np.arange(half, dtype=np.float32) / half)).astype(np.float32)
    angle = np.arange(rows, dtype=np.float32)[:, None] * rate
    cos, sin = np.cos(angle.astype(np.float64)), np.sin(angle.astype(np.float64))
    both = np.stack([np.concatenate([cos, cos], 1), np.concatenate([-sin, sin], 1)]).astype(np.float32)
    return both.reshape(2, rows // HALF, HALF, HEAD)


def solution(mesh):
    any_, vmem = pl.ANY, pltpu.VMEM

    def step(x, gain_a, wq, wk, wv, wo, gain_m, w_gate, w_up, w_down):
        rows, d = x.shape
        dma = lambda *s: pltpu.SemaphoreType.DMA(s)
        four = (2, 4, HALF, WIDE)
        table = jnp.asarray(turns(4 * rows))
        h = call(
            attention_half, "attention_half", 0,
            (x, gain_a.reshape(1, d), table, wq, wk, wv, wo), (any_, vmem) + (any_,) * 5,
            [
                pltpu.VMEM((rows, d), BF), pltpu.VMEM((4, rows, d), BF), pltpu.VMEM((3, d, 512), BF), pltpu.VMEM((4, 1024, WIDE), BF),
                pltpu.VMEM(table.shape, F32), pltpu.VMEM((256, 512), BF), pltpu.VMEM((8, 8, HALF, HEAD), BF), pltpu.VMEM((2, 1024, HEAD), BF),
                pltpu.VMEM((2, HEAD + 16, 1024), BF), pltpu.VMEM((HALF, 1024), BF), pltpu.VMEM((2, 512), F32),
                pltpu.VMEM((2, HEAD + 16, 512), F32), pltpu.VMEM((256, 512), jnp.int32), pltpu.VMEM((2, *four), F32),
                pltpu.VMEM((2, *four), BF), pltpu.VMEM((2, *four), BF), pltpu.VMEM(four, BF), pltpu.VMEM(four, BF), pltpu.VMEM(four, BF),
                dma(2), dma(4), dma(4), dma(2, 2), dma(2, 2), dma(2, 2), dma(2, 2, 2, 4), dma(2, 2, 4), dma(2, 4),
            ],
            x.shape, 26_000_000_000, 28_000_000,
        )
        units = w_gate.shape[1]
        flat = (4, 2 * HALF, WIDE)
        return call(
            mlp_half, "mlp_half", 1,
            (h, gain_m.reshape(1, d), w_gate, w_up, w_down), (any_, vmem, any_, any_, any_),
            [
                pltpu.VMEM((rows, d), BF), pltpu.VMEM((4, rows, d), BF), pltpu.VMEM((2 * rows, units), BF), pltpu.VMEM((rows, units), BF),
                pltpu.VMEM((GU_SLOTS, d, 2 * PART), BF), pltpu.VMEM((D_SLOTS, units, WIDE), BF), pltpu.VMEM((4, HALF, WIDE), F32),
                pltpu.VMEM(four, BF), pltpu.VMEM(four, BF), pltpu.VMEM(four, BF), pltpu.VMEM(four, BF),
                pltpu.VMEM(flat, F32), pltpu.VMEM(flat, BF), pltpu.VMEM(flat, BF), pltpu.VMEM(flat, BF),
                dma(1), dma(GU_SLOTS, 2), dma(D_SLOTS), dma(2, 2), dma(2, 2), dma(2, 2), dma(2, 2, 4), dma(2, 2, 4), dma(2, 4), dma(4),
            ],
            x.shape, 80_000_000_000, 240_000_000,
        )

    tokens, columns, rows_of = P(("dp", "tp"), None), P(None, "tp"), P("tp", None)
    return jax.shard_map(
        step,
        mesh=mesh,
        in_specs=(tokens, P(None), columns, columns, columns, rows_of, P(None), columns, columns, rows_of),
        out_specs=tokens,
        check_vma=False,
    )
```

```python
import jax
import jax.numpy as jnp
import numpy as np
from jax import lax
from jax.experimental import pallas as pl
from jax.experimental.pallas import tpu as pltpu
from jax.sharding import PartitionSpec as P

MESH = pl.DeviceIdType.MESH
BF, F32 = jnp.bfloat16, jnp.float32
HEAD = 128
THETA = 10000
NEG = -1e30
HIDDEN = 2 * NEG
E = HEAD**-0.5 * 1.4426950408889634
HALF = 128
WIDE = 1024
VMEM_LIMIT = 67043328 - 2**21


def dot(a, b):
    return jnp.dot(a, b, preferred_element_type=F32)


class Place:
    def __init__(self):
        tp, dp = lax.axis_index("tp"), lax.axis_index("dp")
        self.c, self.x = lax.rem(tp, 2), lax.div(tp, 2)
        self.partner = (dp, self.x * 2 + (1 - self.c))
        self.across = (dp, (1 - self.x) * 2 + self.c)

    def greet(self):
        barrier = pltpu.get_barrier_semaphore()
        for who in (self.partner, self.across):
            pl.semaphore_signal(barrier, inc=1, device_id=who, device_id_type=MESH)
        pl.semaphore_wait(barrier, 2)


def remote(src, dst, sems, at, who):
    return pltpu.make_async_remote_copy(
        src_ref=src, dst_ref=dst, send_sem=sems.at[(0, *at)], recv_sem=sems.at[(1, *at)], device_id=who, device_id_type=MESH
    )


def norm_into(src, dst, gain, first):
    @pl.loop(0, HALF // 32)
    def _(i):
        rows = pl.ds(pl.multiple_of(first + i * 32, 32), 32)
        wide = src[rows, :].astype(F32)
        scale = lax.rsqrt(jnp.mean(wide * wide, -1, keepdims=True) + 1e-6)
        dst[rows, :] = (wide * scale * gain[...].astype(F32)).astype(BF)


PART = 256
GU_SLOTS, D_SLOTS = 3, 2


def at(i, size):
    return pl.ds(pl.multiple_of(i * size, size), size)


def layer(x_hbm, gain_a, gain_m, tab_hbm, wq, wk, wv, wo, wg, wu, wd, res, a, gu, dn, tab, tq, seen, top, mix, acc,
          ds, dr, xs, xr, hid, load_sem, w_sem, wo_sem, gu_sem, d_sem, own_sem, cross_sem, hand_sem, pair_sem, sum_sem, free_sem):
    place = Place()
    c, x = place.c, place.x
    units = wg.shape[1]
    full = units // PART
    tiles = full + 1
    halves = [pl.ds(k * HALF, HALF) for k in range(2)]
    load = [pltpu.make_async_copy(x_hbm.at[r], res.at[r], load_sem.at[k]) for k, r in enumerate(halves)]
    for w in load:
        w.start()
    load_tab = pltpu.make_async_copy(tab_hbm, tab, load_sem.at[2])
    loads = [
        pltpu.make_async_copy(wq.at[:, 0:512], gu.at[0], w_sem.at[0]),
        pltpu.make_async_copy(wq.at[:, 512:1024], gu.at[1], w_sem.at[1]),
        pltpu.make_async_copy(wk, gu.at[2, :, 0:256], w_sem.at[2]),
        pltpu.make_async_copy(wv, gu.at[2, :, 256:512], w_sem.at[3]),
    ]
    loads_o = [
        pltpu.make_async_copy(wo.at[:, t * WIDE : (t + 1) * WIDE], dn.at[t // 3, pl.ds(t % 3 * 1024, 1024)], wo_sem.at[t]) for t in range(4)
    ]
    mine = at(c, HALF)

    own = [[remote(a.at[0, r], a.at[1, r], own_sem, (f, k), place.partner) for k, r in enumerate(halves)] for f in range(2)]
    cross = [
        [remote(a.at[lax.rem(c + k, 2), mine], a.at[2 + k, mine], cross_sem, (0, k), place.across) for k in range(2)],
        [remote(a.at[0, halves[k]], a.at[2 + k, halves[0]], cross_sem, (1, k), place.across) for k in range(2)],
    ]
    hand = [
        [remote(a.at[2 + k, mine], a.at[2 + k, mine], hand_sem, (0, k), place.partner) for k in range(2)],
        [remote(a.at[2 + k, halves[0]], a.at[2 + k, halves[1]], hand_sem, (1, k), place.partner) for k in range(2)],
    ]
    handed = [
        [remote(a.at[2 + k, at(1 - c, HALF)], a.at[2 + k, at(1 - c, HALF)], hand_sem, (0, k), place.partner) for k in range(2)],
        hand[1],
    ]

    def pair(f, s, k, t):
        return remote(ds.at[s, k, t], dr.at[s, k, t], pair_sem, (f, s, k, t), place.partner)

    def over(f, k, t):
        return remote(xs.at[k, t], xr.at[k, t], sum_sem, (f, k, t), place.across)

    place.greet()
    load[0].wait()
    norm_into(res, a.at[0], gain_a, 0)
    own[0][0].start()

    @pl.when(c == 0)
    def _():
        cross[0][0].start()

    load[1].wait()
    for w in (*loads, load_tab, *loads_o):
        w.start()
    norm_into(res, a.at[0], gain_a, HALF)
    own[0][1].start()
    hid[2] = jnp.zeros(hid.shape[1:], BF)
    hid[2, HEAD : HEAD + 16, 1024:3072] = jnp.ones((16, 2048), BF)

    @pl.when(c == 0)
    def _():
        own[0][0].wait_recv()
        cross[0][1].start()

    @pl.when(c == 1)
    def _():
        own[0][1].wait_recv()
        cross[0][0].start()
        cross[0][1].start()

    load_tab.wait()
    for w in loads:
        w.wait()

    def queries(b):
        return lax.div(b, 6), at(lax.rem(b, 2), HALF), lax.div(lax.rem(b, 6), 2) * 8

    def project(u):
        far = lax.div(u, 2)
        core = c + u * (1 - 2 * c)
        b0 = (1 - far) * (x * 4 + core * 2) + far * ((1 - x) * 4 + (u - 2) * 2)

        @pl.loop(0, 3)
        def _(j):
            tq[...] = dot(a[u], gu[j]).astype(BF)
            for half in range(2):
                b = b0 + half

                def part(n, half=half):
                    return tq[half * HALF : (half + 1) * HALF, n * HEAD : (n + 1) * HEAD]

                def turned(n, b=b, part=part):
                    t = part(n).astype(F32)
                    return (t * tab[0, b] + pltpu.roll(t, HEAD // 2, 1) * tab[1, b]).astype(BF)

                @pl.when(j < 2)
                def _():
                    slot, rows, first = queries(b)
                    for n in range(4):
                        hid[slot, rows, at(first + j * 4 + n, HEAD)] = turned(n)

                @pl.when(j == 2)
                def _():
                    for n in range(2):
                        hid[2, at(lax.rem(b, 2), HALF), at(n * 4 + lax.div(b, 2), HEAD)] = turned(n)
                        hid[2, :HEAD, at(8 + n * 8 + b, HALF)] = part(2 + n).T

    def block(i):
        s, o, k = lax.div(i, 4), lax.div(lax.rem(i, 4), 2), lax.rem(i, 2)
        b = ((1 - s) * (1 - x) + s * x) * 4 + lax.rem(i, 4)
        top[...] = jnp.full_like(top, NEG)
        mix[...] = jnp.zeros_like(mix)
        slot, rows, first = queries(b)

        def query(g):
            return jnp.concatenate([hid[slot, rows, at(first + 4 * g + n, HEAD)] for n in range(4)], axis=0)

        @pl.loop(0, lax.div(b, 2) + 1)
        def _(j):
            gap = lax.rem(lax.broadcasted_iota(jnp.int32, (256, 512), 1), HALF) - lax.broadcasted_iota(jnp.int32, (256, 512), 0)
            ok = gap >= j * 256 - b * HALF
            scores = [
                lax.dot_general(hid[2, :, at(g * 4 + j, HEAD)], query(g), (((1,), (1,)), ((), ())), preferred_element_type=F32)
                for g in range(2)
            ]
            weights, keeps = [], []
            for g in range(2):
                sc = jnp.where(ok, scores[g], HIDDEN)
                old = top[g : g + 1, :]
                new = jnp.maximum(old, sc.max(axis=0, keepdims=True))
                top[g : g + 1, :] = new
                weights.append(jnp.exp2((sc - new) * E).astype(BF))
                keeps.append(jnp.exp2((old - new) * E))
            for g in range(2):
                mix[g] = mix[g] * keeps[g] + dot(hid[2, : HEAD + 16, at(4 + g * 4 + j, 256)], weights[g])

        for g in range(2):
            out = mix[g, :HEAD, :] * (1 / mix[g, HEAD : HEAD + 1, :])
            for n in range(4):
                seen[:, (4 * g + n) * HEAD : (4 * g + n + 1) * HEAD] = out[:, n * HEAD : (n + 1) * HEAD].T.astype(BF)

        is_mine = 1 - lax.rem(o + c, 2)
        into = is_mine * k + (1 - is_mine) * 2
        for t in range(4):
            acc[into, t] = dot(seen[...], dn[t // 3, pl.ds(t % 3 * 1024, 1024), :])

        @pl.when(o != c)
        def _():
            @pl.loop(0, 4)
            def _(t):
                ds[s, k, t] = acc[2, t].astype(BF)
                pair(0, s, k, t).start()

        @pl.when((s == 0) & (o == c))
        def _():
            @pl.loop(0, 4)
            def _(t):
                combine(0, k, t, k)

    def combine(f, k, t, at_k):
        pair(f, 0, k, t).wait_recv()
        xs[k, t] = (acc[at_k, t] + dr[0, k, t].astype(F32)).astype(BF)
        over(f, k, t).start()

    @pl.loop(0, 4)
    def _(u):
        @pl.when(u == 1)
        def _():
            @pl.when(c == 0)
            def _():
                own[0][1].wait_recv()

            @pl.when(c == 1)
            def _():
                own[0][0].wait_recv()

        for k in range(2):

            @pl.when(u == 2 + k)
            def _(k=k):
                cross[0][k].wait_recv()
                hand[0][k].start()
                handed[0][k].wait_recv()
                hand[0][k].wait_send()

        project(u)

        @pl.when(u == 2)
        def _():
            for w in loads_o:
                w.wait()

            @pl.loop(0, 2)
            def _(i):
                block(i)

    def gu_tile(j, slot):
        return [
            pltpu.make_async_copy(wg.at[:, at(j, PART)], gu.at[slot, :, 0:PART], gu_sem.at[slot, 0]),
            pltpu.make_async_copy(wu.at[:, at(j, PART)], gu.at[slot, :, PART : 2 * PART], gu_sem.at[slot, 1]),
        ]

    def gu_last(slot):
        cols, half = pl.ds(full * PART, PART // 2), PART // 2
        return [
            pltpu.make_async_copy(wg.at[:, cols], gu.at[slot, :, 0:half], gu_sem.at[slot, 0]),
            pltpu.make_async_copy(wu.at[:, cols], gu.at[slot, :, half:PART], gu_sem.at[slot, 1]),
        ]

    def d_tile(t):
        slot = lax.rem(t, D_SLOTS)
        return pltpu.make_async_copy(wd.at[:, at(t, WIDE)], dn.at[slot], d_sem.at[slot])

    for j in range(GU_SLOTS):
        for w in gu_tile(j, j):
            w.start()
    for who in (place.partner, place.across):
        pl.semaphore_signal(free_sem, inc=1, device_id=who, device_id_type=MESH)
    for k in range(2):
        own[0][k].wait_send()
        cross[0][k].wait_send()

    def finish(f, k, t):
        pair(f, 1, k, t).wait_recv()
        over(f, k, t).wait_recv()
        rows, cols = at(k, HALF), at(t, WIDE)
        term = acc[k, t] + dr[1, k, t].astype(F32) + xr[k, t].astype(F32)
        res[rows, cols] = (res[rows, cols].astype(F32) + term).astype(BF)

    def own_half(k):
        @pl.loop(0, 4)
        def _(t):
            finish(0, k, t)

        norm_into(res, a.at[0], gain_m, k * HALF)
        own[1][k].start()

    @pl.loop(2, 8)
    def _(i):
        block(i)

        @pl.when(i == 5)
        def _():
            pl.semaphore_wait(free_sem, 2)

        for k in range(2):

            @pl.when((c == 0) & (i == 5 + k))
            def _(k=k):
                own_half(k)

    for t in range(D_SLOTS):
        d_tile(t).start()

    @pl.loop(0, 4)
    def _(p):
        near = 1 - lax.div(p, 2)
        lhs = a.at[near * (c + p * (1 - 2 * c)) + (1 - near) * p]
        k = p - 2
        into = hid.at[near * p + (1 - near) * 2]

        @pl.when((p < 2) & (p != c))
        def _():
            own[1][0].wait_recv()
            own[1][1].wait_recv()

        @pl.when(p == 2)
        def _():
            hand[1][0].wait_recv()

        @pl.when(p == 3)
        def _():
            hand[1][1].wait_recv()

        @pl.loop(0, full)
        def _(j):
            slot = lax.rem(p + j, GU_SLOTS)
            for w in gu_tile(j, slot):
                w.wait()
            r = dot(lhs[...], gu[slot])
            into[:, at(j, PART)] = (jax.nn.silu(r[:, :PART]) * r[:, PART:]).astype(BF)
            later = j + GU_SLOTS

            @pl.when(later < full)
            def _():
                for w in gu_tile(later, slot):
                    w.start()

            @pl.when(later == full)
            def _():
                for w in gu_last(slot):
                    w.start()

            @pl.when((later > full) & (p < 3))
            def _():
                for w in gu_tile(later - tiles, slot):
                    w.start()

            for k in range(2):

                @pl.when((p == 0) & (c == 0) & (j == 5 + 4 * k))
                def _(k=k):
                    cross[1][k].start()

                @pl.when((p == 0) & (c == 1) & (j == 3 + 7 * k))
                def _(k=k):
                    own_half(k)
                    cross[1][k].start()

            @pl.when((p == 3) & (j == 1))
            def _():
                combine(1, 0, 3, 2)

        slot = lax.rem(p + full, GU_SLOTS)
        for w in gu_last(slot):
            w.wait()
        r = dot(lhs[...], gu[slot, :, 0:PART])
        into[:, full * PART :] = (jax.nn.silu(r[:, : PART // 2]) * r[:, PART // 2 :]).astype(BF)

        @pl.when(p < 3)
        def _():
            for w in gu_tile(GU_SLOTS - 1, slot):
                w.start()

        @pl.when(p == 1)
        def _():
            cross[1][0].wait_recv()
            hand[1][0].start()

            @pl.loop(0, 8)
            def _(i):
                kk, t = lax.div(i, 4), lax.rem(i, 4)
                over(0, kk, t).wait_send()
                pair(0, 0, kk, t).wait_send()
                pair(0, 1, kk, t).wait_send()

        @pl.when(p >= 2)
        def _():
            @pl.loop(0, 4)
            def _(t):
                d_tile(t).wait()
                r = dot(into[...], dn[lax.rem(t, D_SLOTS)])
                d_tile(lax.rem(t + D_SLOTS, 4)).start()
                acc[2, t] = r[:HALF]
                ds[0, k, t] = r[HALF:].astype(BF)
                pair(1, 0, k, t).start()

                @pl.when(t > 0)
                def _():
                    combine(1, k, t - 1, 2)

                @pl.when((p == 2) & (t == 1))
                def _():
                    cross[1][1].wait_recv()
                    hand[1][1].start()

    def finish_tile(t):
        for k in range(2):
            finish(1, k, t)

    @pl.loop(0, 4)
    def _(t):
        d_tile(t).wait()
        w = dn.at[lax.rem(t, D_SLOTS)]
        r = dot(hid[1 - c], w[...])
        for k in range(2):
            ds[1, k, t] = r[k * HALF : (k + 1) * HALF].astype(BF)
            pair(1, 1, k, t).start()
        r = dot(hid[c], w[...])
        for k in range(2):
            acc[k, t] = r[k * HALF : (k + 1) * HALF]

        @pl.when(t == 0)
        def _():
            combine(1, 1, 3, 2)

        @pl.when(t < 4 - D_SLOTS)
        def _():
            d_tile(t + D_SLOTS).start()

        @pl.when(t > 0)
        def _():
            finish_tile(t - 1)

    finish_tile(3)

    @pl.loop(0, 8)
    def _(i):
        k, t = lax.div(i, 4), lax.rem(i, 4)
        over(1, k, t).wait_send()
        pair(1, 0, k, t).wait_send()
        pair(1, 1, k, t).wait_send()

    for k in range(2):
        own[1][k].wait_send()
        cross[1][k].wait_send()
        hand[1][k].wait_send()


def turns(rows):
    half = HEAD // 2
    rate = (float(THETA) ** (-np.arange(half, dtype=np.float32) / half)).astype(np.float32)
    angle = np.arange(rows, dtype=np.float32)[:, None] * rate
    cos, sin = np.cos(angle.astype(np.float64)), np.sin(angle.astype(np.float64))
    both = np.stack([np.concatenate([cos, cos], 1), np.concatenate([-sin, sin], 1)]).astype(np.float32)
    return both.reshape(2, rows // HALF, HALF, HEAD)


def solution(mesh):
    def step(x, gain_a, wq, wk, wv, wo, gain_m, w_gate, w_up, w_down):
        rows, d = x.shape
        units = w_gate.shape[1]
        dma = lambda *s: pltpu.SemaphoreType.DMA(s)
        tiles = (2, 4, HALF, WIDE)
        table = jnp.asarray(turns(4 * rows))
        anywhere, vmem = pl.BlockSpec(memory_space=pl.ANY), pl.BlockSpec(memory_space=pltpu.VMEM)
        return pl.pallas_call(
            layer,
            out_shape=pltpu.VMEM(x.shape, BF),
            in_specs=[anywhere, vmem, vmem] + [anywhere] * 8,
            out_specs=vmem,
            scratch_shapes=[
                pltpu.VMEM((4, rows, d), BF), pltpu.VMEM((GU_SLOTS, d, 2 * PART), BF),
                pltpu.VMEM((D_SLOTS, units, WIDE), BF), pltpu.VMEM(table.shape, F32), pltpu.VMEM((256, 512), BF),
                pltpu.VMEM((HALF, 1024), BF), pltpu.VMEM((2, 512), F32), pltpu.VMEM((2, HEAD + 16, 512), F32),
                pltpu.VMEM((3, *tiles[1:]), F32),
                pltpu.VMEM((2, *tiles), BF), pltpu.VMEM((2, *tiles), BF), pltpu.VMEM(tiles, BF), pltpu.VMEM(tiles, BF),
                pltpu.VMEM((3, rows, units), BF),
                dma(3), dma(4), dma(4), dma(GU_SLOTS, 2), dma(D_SLOTS), dma(2, 2, 2), dma(2, 2, 2), dma(2, 2, 2), dma(2, 2, 2, 2, 4),
                dma(2, 2, 2, 4), pltpu.SemaphoreType.REGULAR,
            ],
            compiler_params=pltpu.CompilerParams(collective_id=0, has_side_effects=True, vmem_limit_bytes=VMEM_LIMIT),
            cost_estimate=pl.CostEstimate(flops=104_000_000_000, bytes_accessed=320_000_000, transcendentals=0),
            name="layer",
        )(x, gain_a, gain_m, table, wq, wk, wv, wo, w_gate, w_up, w_down)

    tokens, columns, rows_of = P(("dp", "tp"), None), P(None, "tp"), P("tp", None)
    return jax.shard_map(
        step,
        mesh=mesh,
        in_specs=(tokens, P(None), columns, columns, columns, rows_of, P(None), columns, columns, rows_of),
        out_specs=tokens,
        check_vma=False,
    )
```

```python
import jax
import jax.numpy as jnp
import numpy as np
from jax import lax
from jax.experimental import pallas as pl
from jax.experimental.pallas import tpu as pltpu
from jax.sharding import PartitionSpec as P

MESH = pl.DeviceIdType.MESH
BF, F32 = jnp.bfloat16, jnp.float32
HEAD = 128
THETA = 10000
NEG = -1e30
HIDDEN = 2 * NEG
E = HEAD**-0.5 * 1.4426950408889634
HALF = 128
PIECE = HALF // 2
WIDE = 1024
VMEM_LIMIT = 67043328 - 2**21


def dot(a, b):
    return jnp.dot(a, b, preferred_element_type=F32)


class Place:
    def __init__(self):
        tp, dp = lax.axis_index("tp"), lax.axis_index("dp")
        self.c, self.x = lax.rem(tp, 2), lax.div(tp, 2)
        self.partner = (dp, self.x * 2 + (1 - self.c))
        self.across = (dp, (1 - self.x) * 2 + self.c)

    def greet(self):
        barrier = pltpu.get_barrier_semaphore()
        for who in (self.partner, self.across):
            pl.semaphore_signal(barrier, inc=1, device_id=who, device_id_type=MESH)
        pl.semaphore_wait(barrier, 2)


def remote(src, dst, sems, at, who):
    return pltpu.make_async_remote_copy(
        src_ref=src, dst_ref=dst, send_sem=sems.at[(0, *at)], recv_sem=sems.at[(1, *at)], device_id=who, device_id_type=MESH
    )


def norm_into(src, dst, gain, first):
    @pl.loop(0, HALF // 32)
    def _(i):
        rows = pl.ds(pl.multiple_of(first + i * 32, 32), 32)
        wide = src[rows, :].astype(F32)
        scale = lax.rsqrt(jnp.mean(wide * wide, -1, keepdims=True) + 1e-6)
        dst[rows, :] = (wide * scale * gain[...].astype(F32)).astype(BF)


PART = 256
GU_SLOTS, D_SLOTS = 3, 2
D_PARTS = 4


def at(i, size):
    return pl.ds(pl.multiple_of(i * size, size), size)


def layer(x_hbm, gain_a, gain_m, tab_hbm, wq, wk, wv, wo, wg, wu, wd, res, a, gu, dn, tab, tq, seen, top, mix, acc,
          ds, dr, xs, xr, hid, load_sem, w_sem, wo_sem, gu_sem, d_sem, own_sem, cross_sem, hand_sem, pair_sem, sum_sem, free_sem):
    place = Place()
    c, x = place.c, place.x
    units = wg.shape[1]
    full = units // PART
    tiles = full + 1
    halves = [pl.ds(k * HALF, HALF) for k in range(2)]
    load = [pltpu.make_async_copy(x_hbm.at[r], res.at[r], load_sem.at[k]) for k, r in enumerate(halves)]
    for w in load:
        w.start()
    load_tab = pltpu.make_async_copy(tab_hbm, tab, load_sem.at[2])
    loads = [
        pltpu.make_async_copy(wq.at[:, 0:512], gu.at[0], w_sem.at[0]),
        pltpu.make_async_copy(wq.at[:, 512:1024], gu.at[1], w_sem.at[1]),
        pltpu.make_async_copy(wk, gu.at[2, :, 0:256], w_sem.at[2]),
        pltpu.make_async_copy(wv, gu.at[2, :, 256:512], w_sem.at[3]),
    ]
    loads_o = [
        pltpu.make_async_copy(wo.at[:, t * WIDE : (t + 1) * WIDE], dn.at[t // 3, pl.ds(t % 3 * 1024, 1024)], wo_sem.at[t]) for t in range(4)
    ]

    def pieces(half):
        return [pl.ds(pl.multiple_of(half * HALF + n * PIECE, PIECE), PIECE) for n in range(2)]

    def copies(src, dst, src_half, dst_half, sems, f, k, who):
        rows = zip(pieces(src_half), pieces(dst_half), strict=True)
        return [remote(a.at[src, r], a.at[dst, q], sems, (f, k, n), who) for n, (r, q) in enumerate(rows)]

    own = [[remote(a.at[0, r], a.at[1, r], own_sem, (f, k), place.partner) for k, r in enumerate(halves)] for f in range(2)]
    cross = [
        [copies(lax.rem(c + k, 2), 2 + k, c, c, cross_sem, 0, k, place.across) for k in range(2)],
        [copies(0, 2 + k, k, 0, cross_sem, 1, k, place.across) for k in range(2)],
    ]
    hand = [
        [copies(2 + k, 2 + k, c, c, hand_sem, 0, k, place.partner) for k in range(2)],
        [copies(2 + k, 2 + k, 0, 1, hand_sem, 1, k, place.partner) for k in range(2)],
    ]
    handed = [[copies(2 + k, 2 + k, 1 - c, 1 - c, hand_sem, 0, k, place.partner) for k in range(2)], hand[1]]

    def pass_on(f, k, n):
        cross[f][k][n].wait_recv()
        hand[f][k][n].start()

    def begin(copies):
        for w in copies:
            w.start()

    def received(copies):
        for w in copies:
            w.wait_recv()

    def sent(copies):
        for w in copies:
            w.wait_send()

    def await_(copies):
        for w in copies:
            w.wait()

    def pair(f, s, k, t):
        return remote(ds.at[s, k, t], dr.at[s, k, t], pair_sem, (f, s, k, t), place.partner)

    def over(f, k, t):
        return remote(xs.at[k, t], xr.at[k, t], sum_sem, (f, k, t), place.across)

    place.greet()
    load[0].wait()
    norm_into(res, a.at[0], gain_a, 0)
    own[0][0].start()

    @pl.when(c == 0)
    def _():
        begin(cross[0][0])

    load[1].wait()
    for w in (*loads, load_tab, *loads_o):
        w.start()
    norm_into(res, a.at[0], gain_a, HALF)
    own[0][1].start()
    hid[2] = jnp.zeros(hid.shape[1:], BF)
    hid[2, HEAD : HEAD + 16, 1024:3072] = jnp.ones((16, 2048), BF)

    @pl.when(c == 0)
    def _():
        own[0][0].wait_recv()
        begin(cross[0][1])

    @pl.when(c == 1)
    def _():
        own[0][1].wait_recv()
        begin(cross[0][0])
        begin(cross[0][1])

    load_tab.wait()
    for w in loads:
        w.wait()

    def queries(b):
        return lax.div(b, 6), at(lax.rem(b, 2), HALF), lax.div(lax.rem(b, 6), 2) * 8

    def project(u):
        far = lax.div(u, 2)
        core = c + u * (1 - 2 * c)
        b0 = (1 - far) * (x * 4 + core * 2) + far * ((1 - x) * 4 + (u - 2) * 2)

        @pl.loop(0, 3)
        def _(j):
            tq[...] = dot(a[u], gu[j]).astype(BF)
            for half in range(2):
                b = b0 + half

                def part(n, half=half):
                    return tq[half * HALF : (half + 1) * HALF, n * HEAD : (n + 1) * HEAD]

                def turned(n, b=b, part=part):
                    t = part(n).astype(F32)
                    return (t * tab[0, b] + pltpu.roll(t, HEAD // 2, 1) * tab[1, b]).astype(BF)

                @pl.when(j < 2)
                def _():
                    slot, rows, first = queries(b)
                    for n in range(4):
                        hid[slot, rows, at(first + j * 4 + n, HEAD)] = turned(n)

                @pl.when(j == 2)
                def _():
                    for n in range(2):
                        hid[2, at(lax.rem(b, 2), HALF), at(n * 4 + lax.div(b, 2), HEAD)] = turned(n)
                        hid[2, :HEAD, at(8 + n * 8 + b, HALF)] = part(2 + n).T

    def block(i):
        s, o, k = lax.div(i, 4), lax.div(lax.rem(i, 4), 2), lax.rem(i, 2)
        b = ((1 - s) * (1 - x) + s * x) * 4 + lax.rem(i, 4)
        top[...] = jnp.full_like(top, NEG)
        mix[...] = jnp.zeros_like(mix)
        slot, rows, first = queries(b)

        def query(g):
            return jnp.concatenate([hid[slot, rows, at(first + 4 * g + n, HEAD)] for n in range(4)], axis=0)

        def keys(j, masked):
            if masked:
                gap = lax.rem(lax.broadcasted_iota(jnp.int32, (256, 512), 1), HALF) - lax.broadcasted_iota(jnp.int32, (256, 512), 0)
                ok = gap >= j * 256 - b * HALF
            scores = [
                lax.dot_general(hid[2, :, at(g * 4 + j, HEAD)], query(g), (((1,), (1,)), ((), ())), preferred_element_type=F32)
                for g in range(2)
            ]
            weights, keeps = [], []
            for g in range(2):
                sc = jnp.where(ok, scores[g], HIDDEN) if masked else scores[g]
                old = top[g : g + 1, :]
                new = jnp.maximum(old, sc.max(axis=0, keepdims=True))
                top[g : g + 1, :] = new
                weights.append(jnp.exp2((sc - new) * E).astype(BF))
                keeps.append(jnp.exp2((old - new) * E))
            for g in range(2):
                mix[g] = mix[g] * keeps[g] + dot(hid[2, : HEAD + 16, at(4 + g * 4 + j, 256)], weights[g])

        pl.loop(0, lax.div(b, 2))(lambda j: keys(j, False))
        keys(lax.div(b, 2), True)

        for g in range(2):
            out = mix[g, :HEAD, :] * (1 / mix[g, HEAD : HEAD + 1, :])
            for n in range(4):
                seen[:, (4 * g + n) * HEAD : (4 * g + n + 1) * HEAD] = out[:, n * HEAD : (n + 1) * HEAD].T.astype(BF)

        is_mine = 1 - lax.rem(o + c, 2)
        into = is_mine * k + (1 - is_mine) * 2
        for t in range(4):
            acc[into, t] = dot(seen[...], dn[t // 3, pl.ds(t % 3 * 1024, 1024), :])

        @pl.when(o != c)
        def _():
            @pl.loop(0, 4)
            def _(t):
                ds[s, k, t] = acc[2, t].astype(BF)
                pair(0, s, k, t).start()

        @pl.when((s == 0) & (o == c))
        def _():
            @pl.loop(0, 4)
            def _(t):
                combine(0, k, t, k)

    def combine(f, k, t, at_k):
        pair(f, 0, k, t).wait_recv()
        xs[k, t] = (acc[at_k, t] + dr[0, k, t].astype(F32)).astype(BF)
        over(f, k, t).start()

    @pl.loop(0, 4)
    def _(u):
        @pl.when(u == 1)
        def _():
            @pl.when(c == 0)
            def _():
                own[0][1].wait_recv()

            @pl.when(c == 1)
            def _():
                own[0][0].wait_recv()

        for k in range(2):

            @pl.when(u == 2 + k)
            def _(k=k):
                for n in range(2):
                    pass_on(0, k, n)
                received(handed[0][k])
                sent(hand[0][k])

        project(u)

        @pl.when(u == 2)
        def _():
            for w in loads_o:
                w.wait()

            @pl.loop(0, 2)
            def _(i):
                block(i)

    def gu_tile(j, slot):
        return [
            pltpu.make_async_copy(wg.at[:, at(j, PART)], gu.at[slot, :, 0:PART], gu_sem.at[slot, 0]),
            pltpu.make_async_copy(wu.at[:, at(j, PART)], gu.at[slot, :, PART : 2 * PART], gu_sem.at[slot, 1]),
        ]

    def gu_last(slot):
        cols, half = pl.ds(full * PART, PART // 2), PART // 2
        return [
            pltpu.make_async_copy(wg.at[:, cols], gu.at[slot, :, 0:half], gu_sem.at[slot, 0]),
            pltpu.make_async_copy(wu.at[:, cols], gu.at[slot, :, half:PART], gu_sem.at[slot, 1]),
        ]

    def d_tile(t):
        slot = lax.rem(t, D_SLOTS)
        rows = [pl.ds(i * units // D_PARTS, units // D_PARTS) for i in range(D_PARTS)]
        return [pltpu.make_async_copy(wd.at[r, at(t, WIDE)], dn.at[slot, r], d_sem.at[slot, i]) for i, r in enumerate(rows)]


    for j in range(GU_SLOTS):
        for w in gu_tile(j, j):
            w.start()
    for who in (place.partner, place.across):
        pl.semaphore_signal(free_sem, inc=1, device_id=who, device_id_type=MESH)
    for k in range(2):
        own[0][k].wait_send()
        sent(cross[0][k])

    def finish(f, k, t):
        pair(f, 1, k, t).wait_recv()
        over(f, k, t).wait_recv()
        rows, cols = at(k, HALF), at(t, WIDE)
        term = acc[k, t] + dr[1, k, t].astype(F32) + xr[k, t].astype(F32)
        res[rows, cols] = (res[rows, cols].astype(F32) + term).astype(BF)

    def own_half(k):
        @pl.loop(0, 4)
        def _(t):
            finish(0, k, t)

        norm_into(res, a.at[0], gain_m, k * HALF)
        own[1][k].start()

    @pl.loop(2, 8)
    def _(i):
        block(i)

        @pl.when(i == 5)
        def _():
            pl.semaphore_wait(free_sem, 2)

        for k in range(2):

            @pl.when((c == 0) & (i == 5 + k))
            def _(k=k):
                own_half(k)

    def last_tile(lhs, into):
        r = dot(lhs[...], gu[full % GU_SLOTS, :, 0:PART])
        into[:, full * PART :] = (jax.nn.silu(r[:, : PART // 2]) * r[:, PART // 2 :]).astype(BF)

    @pl.loop(0, 4)
    def _(p):
        near, odd = 1 - lax.div(p, 2), lax.rem(p, 2)
        lhs = a.at[near * (c + p * (1 - 2 * c)) + (1 - near) * p]
        k = p - 2
        into = hid.at[near * p + (1 - near) * 2]

        @pl.when((p < 2) & (p != c))
        def _():
            own[1][0].wait_recv()
            own[1][1].wait_recv()

        @pl.when(p == 2)
        def _():
            received(hand[1][0])

        @pl.when(p == 3)
        def _():
            received(hand[1][1])

        @pl.when(odd == 1)
        def _():
            last_tile(lhs, into)
            begin(gu_tile(full - GU_SLOTS, full % GU_SLOTS))

        @pl.loop(0, full)
        def _(j):
            i = (1 - odd) * j + odd * (full - 1 - j)
            slot = lax.rem(i, GU_SLOTS)

            @pl.when((p == 0) | (j + odd >= GU_SLOTS))
            def _():
                await_(gu_tile(i, slot))

            r = dot(lhs[...], gu[slot])
            into[:, at(i, PART)] = (jax.nn.silu(r[:, :PART]) * r[:, PART:]).astype(BF)

            @pl.when((odd == 0) & (i + GU_SLOTS < full))
            def _():
                begin(gu_tile(i + GU_SLOTS, slot))

            @pl.when((odd == 0) & (i + GU_SLOTS == full))
            def _():
                begin(gu_last(slot))

            @pl.when((odd == 1) & (i >= GU_SLOTS))
            def _():
                begin(gu_tile(i - GU_SLOTS, slot))

            @pl.when((p == 0) & (j == full - 2))
            def _():
                for t in range(D_SLOTS):
                    begin(d_tile(t))

            for k in range(2):

                @pl.when((p == 0) & (c == 0) & (j == 5 + 4 * k))
                def _(k=k):
                    begin(cross[1][k])

                @pl.when((p == 0) & (c == 1) & (j == 3 + 7 * k))
                def _(k=k):
                    own_half(k)
                    begin(cross[1][k])

            for n in range(2):

                @pl.when((p == 1) & (j == full - 3 + 2 * n))
                def _(n=n):
                    pass_on(1, 0, n)

            @pl.when((p == 3) & (j == 1))
            def _():
                combine(1, 0, 3, 2)

        @pl.when(odd == 0)
        def _():
            await_(gu_last(full % GU_SLOTS))
            last_tile(lhs, into)

        @pl.when(p == 1)
        def _():
            @pl.loop(0, 8)
            def _(i):
                kk, t = lax.div(i, 4), lax.rem(i, 4)
                over(0, kk, t).wait_send()
                pair(0, 0, kk, t).wait_send()
                pair(0, 1, kk, t).wait_send()

        @pl.when(p >= 2)
        def _():
            @pl.loop(0, 4)
            def _(q):
                t = (1 - k) * q + k * (3 - q)

                @pl.when((k == 0) | (q >= D_SLOTS))
                def _():
                    await_(d_tile(t))

                r = dot(into[...], dn[lax.rem(t, D_SLOTS)])

                @pl.when((k == 0) & (q < 2))
                def _():
                    begin(d_tile(t + 2))

                @pl.when(k == 1)
                def _():
                    begin(d_tile(lax.rem(t + 2, 4)))

                acc[2, t] = r[:HALF]
                ds[0, k, t] = r[HALF:].astype(BF)
                pair(1, 0, k, t).start()

                @pl.when(q > 0)
                def _():
                    combine(1, k, t - 1 + 2 * k, 2)

                @pl.when((p == 2) & (q == 1))
                def _():
                    for n in range(2):
                        pass_on(1, 1, n)

    def finish_tile(t):
        for k in range(2):
            finish(1, k, t)

    @pl.loop(0, 4)
    def _(q):
        t = 3 - q
        await_(d_tile(t))
        w = dn.at[lax.rem(t, D_SLOTS)]
        r = dot(hid[1 - c], w[...])
        for k in range(2):
            ds[1, k, t] = r[k * HALF : (k + 1) * HALF].astype(BF)
            pair(1, 1, k, t).start()

        @pl.when(q == 0)
        def _():
            combine(1, 1, 0, 2)

        r = dot(hid[c], w[...])
        for k in range(2):
            acc[k, t] = r[k * HALF : (k + 1) * HALF]

        @pl.when(q < 4 - D_SLOTS)
        def _():
            begin(d_tile(t - D_SLOTS))

        @pl.when(q > 0)
        def _():
            finish_tile(t + 1)

    finish_tile(0)

    @pl.loop(0, 8)
    def _(i):
        k, t = lax.div(i, 4), lax.rem(i, 4)
        over(1, k, t).wait_send()
        pair(1, 0, k, t).wait_send()
        pair(1, 1, k, t).wait_send()

    for k in range(2):
        own[1][k].wait_send()
        sent(cross[1][k])
        sent(hand[1][k])


def turns(rows):
    half = HEAD // 2
    rate = (float(THETA) ** (-np.arange(half, dtype=np.float32) / half)).astype(np.float32)
    angle = np.arange(rows, dtype=np.float32)[:, None] * rate
    cos, sin = np.cos(angle.astype(np.float64)), np.sin(angle.astype(np.float64))
    both = np.stack([np.concatenate([cos, cos], 1), np.concatenate([-sin, sin], 1)]).astype(np.float32)
    return both.reshape(2, rows // HALF, HALF, HEAD)


def solution(mesh):
    def step(x, gain_a, wq, wk, wv, wo, gain_m, w_gate, w_up, w_down):
        rows, d = x.shape
        units = w_gate.shape[1]
        dma = lambda *s: pltpu.SemaphoreType.DMA(s)
        tiles = (2, 4, HALF, WIDE)
        table = jnp.asarray(turns(4 * rows))
        anywhere, vmem = pl.BlockSpec(memory_space=pl.ANY), pl.BlockSpec(memory_space=pltpu.VMEM)
        return pl.pallas_call(
            layer,
            out_shape=pltpu.VMEM(x.shape, BF),
            in_specs=[anywhere, vmem, vmem] + [anywhere] * 8,
            out_specs=vmem,
            scratch_shapes=[
                pltpu.VMEM((4, rows, d), BF), pltpu.VMEM((GU_SLOTS, d, 2 * PART), BF),
                pltpu.VMEM((D_SLOTS, units, WIDE), BF), pltpu.VMEM(table.shape, F32), pltpu.VMEM((256, 512), BF),
                pltpu.VMEM((HALF, 1024), BF), pltpu.VMEM((2, 512), F32), pltpu.VMEM((2, HEAD + 16, 512), F32),
                pltpu.VMEM((3, *tiles[1:]), F32),
                pltpu.VMEM((2, *tiles), BF), pltpu.VMEM((2, *tiles), BF), pltpu.VMEM(tiles, BF), pltpu.VMEM(tiles, BF),
                pltpu.VMEM((3, rows, units), BF),
                dma(3), dma(4), dma(4), dma(GU_SLOTS, 2), dma(D_SLOTS, D_PARTS), dma(2, 2, 2), dma(2, 2, 2, 2), dma(2, 2, 2, 2), dma(2, 2, 2, 2, 4),
                dma(2, 2, 2, 4), pltpu.SemaphoreType.REGULAR,
            ],
            compiler_params=pltpu.CompilerParams(collective_id=0, has_side_effects=True, vmem_limit_bytes=VMEM_LIMIT),
            cost_estimate=pl.CostEstimate(flops=104_000_000_000, bytes_accessed=320_000_000, transcendentals=0),
            name="layer",
        )(x, gain_a, gain_m, table, wq, wk, wv, wo, w_gate, w_up, w_down)

    tokens, columns, rows_of = P(("dp", "tp"), None), P(None, "tp"), P("tp", None)
    return jax.shard_map(
        step,
        mesh=mesh,
        in_specs=(tokens, P(None), columns, columns, columns, rows_of, P(None), columns, columns, rows_of),
        out_specs=tokens,
        check_vma=False,
    )
```

```python
import jax
import jax.numpy as jnp
import numpy as np
from jax import lax
from jax.experimental import pallas as pl
from jax.experimental.pallas import tpu as pltpu
from jax.sharding import PartitionSpec as P

MESH = pl.DeviceIdType.MESH
BF, F32 = jnp.bfloat16, jnp.float32
HEAD = 128
THETA = 10000
NEG = -1e30
HIDDEN = 2 * NEG
E = HEAD**-0.5 * 1.4426950408889634
HALF = 128
PIECE = HALF // 2
WIDE = 1024
VMEM_LIMIT = 67043328 - 2**21


def dot(a, b):
    return jnp.dot(a, b, preferred_element_type=F32)


class Place:
    def __init__(self):
        tp, dp = lax.axis_index("tp"), lax.axis_index("dp")
        self.c, self.x, self.dp = lax.rem(tp, 2), lax.div(tp, 2), dp
        self.partner = (dp, self.x * 2 + (1 - self.c))
        self.across = (dp, (1 - self.x) * 2 + self.c)

    def greet(self):
        barrier = pltpu.get_barrier_semaphore()
        for who in (self.partner, self.across, self.far(1 - self.c)):
            pl.semaphore_signal(barrier, inc=1, device_id=who, device_id_type=MESH)
        pl.semaphore_wait(barrier, 3)

    def far(self, core):
        return self.dp, (1 - self.x) * 2 + core


def remote(src, dst, sems, at, who):
    return pltpu.make_async_remote_copy(
        src_ref=src, dst_ref=dst, send_sem=sems.at[(0, *at)], recv_sem=sems.at[(1, *at)], device_id=who, device_id_type=MESH
    )


def norm_into(src, dst, gain, first, count=HALF):
    @pl.loop(0, count // 32)
    def _(i):
        rows = pl.ds(pl.multiple_of(first + i * 32, 32), 32)
        wide = src[rows, :].astype(F32)
        scale = lax.rsqrt(jnp.mean(wide * wide, -1, keepdims=True) + 1e-6)
        dst[rows, :] = (wide * scale * gain[...].astype(F32)).astype(BF)


PART = 256
GU_SLOTS, D_SLOTS = 3, 2
D_PARTS = 4


def at(i, size):
    return pl.ds(pl.multiple_of(i * size, size), size)


def layer(x_hbm, gain_a, gain_m, tab_hbm, wq, wk, wv, wo, wg, wu, wd, res, a, gu, dn, tab, tq, seen, top, mix, acc,
          ds, dr, xs, xr, hid, load_sem, w_sem, wo_sem, gu_sem, d_sem, own_sem, cross_sem, hand_sem, pair_sem, sum_sem, free_sem):
    place = Place()
    c, x = place.c, place.x
    units = wg.shape[1]
    full = units // PART
    tiles = full + 1
    halves = [pl.ds(k * HALF, HALF) for k in range(2)]
    load = [pltpu.make_async_copy(x_hbm.at[r], res.at[r], load_sem.at[k]) for k, r in enumerate(halves)]
    for w in load:
        w.start()
    load_tab = pltpu.make_async_copy(tab_hbm, tab, load_sem.at[2])
    loads = [
        pltpu.make_async_copy(wq.at[:, 0:512], gu.at[0], w_sem.at[0]),
        pltpu.make_async_copy(wq.at[:, 512:1024], gu.at[1], w_sem.at[1]),
        pltpu.make_async_copy(wk, gu.at[2, :, 0:256], w_sem.at[2]),
        pltpu.make_async_copy(wv, gu.at[2, :, 256:512], w_sem.at[3]),
    ]
    loads_o = [
        pltpu.make_async_copy(wo.at[:, t * WIDE : (t + 1) * WIDE], dn.at[t // 3, pl.ds(t % 3 * 1024, 1024)], wo_sem.at[t]) for t in range(4)
    ]

    def pieces(half):
        return [pl.ds(pl.multiple_of(half * HALF + n * PIECE, PIECE), PIECE) for n in range(2)]

    def copies(src, dst, src_half, dst_half, sems, f, k, who):
        rows = zip(pieces(src_half), pieces(dst_half), strict=True)
        return [remote(a.at[src, r], a.at[dst, q], sems, (f, k, n), who) for n, (r, q) in enumerate(rows)]

    own = [[remote(a.at[0, r], a.at[1, r], own_sem, (f, k), place.partner) for k, r in enumerate(halves)] for f in range(2)]
    cross = [
        [copies(lax.rem(c + k, 2), 2 + k, c, c, cross_sem, 0, k, place.across) for k in range(2)],
        [copies(0, 2 + k, k, 0, cross_sem, 1, k, place.across) for k in range(2)],
    ]
    hand = [
        [copies(2 + k, 2 + k, c, c, hand_sem, 0, k, place.partner) for k in range(2)],
        [copies(2 + k, 2 + k, 0, 1, hand_sem, 1, k, place.partner) for k in range(2)],
    ]
    handed = [[copies(2 + k, 2 + k, 1 - c, 1 - c, hand_sem, 0, k, place.partner) for k in range(2)], hand[1]]

    def pass_on(f, k, n):
        cross[f][k][n].wait_recv()
        hand[f][k][n].start()

    def begin(copies):
        for w in copies:
            w.start()

    def received(copies):
        for w in copies:
            w.wait_recv()

    def sent(copies):
        for w in copies:
            w.wait_send()

    def await_(copies):
        for w in copies:
            w.wait()

    def pair(f, s, k, t):
        return remote(ds.at[s, k, t], dr.at[s, k, t], pair_sem, (f, s, k, t), place.partner)

    def over(f, k, t):
        return remote(xs.at[k, t], xr.at[k, t], sum_sem, (f, k, t), place.across)

    place.greet()
    load[0].wait()
    for n in range(2):
        norm_into(res, a.at[0], gain_a, n * PIECE, PIECE)

        @pl.when(c == 0)
        def _(n=n):
            cross[0][0][n].start()

    own[0][0].start()

    load[1].wait()
    for w in (*loads, load_tab, *loads_o):
        w.start()
    norm_into(res, a.at[0], gain_a, HALF)
    own[0][1].start()
    hid[2] = jnp.zeros(hid.shape[1:], BF)
    hid[2, HEAD : HEAD + 16, 1024:3072] = jnp.ones((16, 2048), BF)

    @pl.when(c == 0)
    def _():
        own[0][0].wait_recv()
        begin(cross[0][1])

    @pl.when(c == 1)
    def _():
        own[0][1].wait_recv()
        begin(cross[0][0])
        begin(cross[0][1])

    load_tab.wait()
    for w in loads:
        w.wait()

    def queries(b):
        return lax.div(b, 6), at(lax.rem(b, 2), HALF), lax.div(lax.rem(b, 6), 2) * 8

    def project(u):
        far = lax.div(u, 2)
        core = c + u * (1 - 2 * c)
        b0 = (1 - far) * (x * 4 + core * 2) + far * ((1 - x) * 4 + (u - 2) * 2)

        @pl.loop(0, 3)
        def _(j):
            tq[...] = dot(a[u], gu[j]).astype(BF)
            for half in range(2):
                b = b0 + half

                def part(n, half=half):
                    return tq[half * HALF : (half + 1) * HALF, n * HEAD : (n + 1) * HEAD]

                def turned(n, b=b, part=part):
                    t = part(n).astype(F32)
                    return (t * tab[0, b] + pltpu.roll(t, HEAD // 2, 1) * tab[1, b]).astype(BF)

                @pl.when(j < 2)
                def _():
                    slot, rows, first = queries(b)
                    for n in range(4):
                        hid[slot, rows, at(first + j * 4 + n, HEAD)] = turned(n)

                @pl.when(j == 2)
                def _():
                    for n in range(2):
                        hid[2, at(lax.rem(b, 2), HALF), at(n * 4 + lax.div(b, 2), HEAD)] = turned(n)
                        hid[2, :HEAD, at(8 + n * 8 + b, HALF)] = part(2 + n).T

    def block(i):
        s, o, k = lax.div(i, 4), lax.div(lax.rem(i, 4), 2), lax.rem(i, 2)
        b = ((1 - s) * (1 - x) + s * x) * 4 + lax.rem(i, 4)
        top[...] = jnp.full_like(top, NEG)
        mix[...] = jnp.zeros_like(mix)
        slot, rows, first = queries(b)

        def query(g):
            return jnp.concatenate([hid[slot, rows, at(first + 4 * g + n, HEAD)] for n in range(4)], axis=0)

        def keys(j, masked):
            if masked:
                gap = lax.rem(lax.broadcasted_iota(jnp.int32, (256, 512), 1), HALF) - lax.broadcasted_iota(jnp.int32, (256, 512), 0)
                ok = gap >= j * 256 - b * HALF
            scores = [
                lax.dot_general(hid[2, :, at(g * 4 + j, HEAD)], query(g), (((1,), (1,)), ((), ())), preferred_element_type=F32)
                for g in range(2)
            ]
            weights, keeps = [], []
            for g in range(2):
                sc = jnp.where(ok, scores[g], HIDDEN) if masked else scores[g]
                old = top[g : g + 1, :]
                new = jnp.maximum(old, sc.max(axis=0, keepdims=True))
                top[g : g + 1, :] = new
                weights.append(jnp.exp2((sc - new) * E).astype(BF))
                keeps.append(jnp.exp2((old - new) * E))
            for g in range(2):
                mix[g] = mix[g] * keeps[g] + dot(hid[2, : HEAD + 16, at(4 + g * 4 + j, 256)], weights[g])

        pl.loop(0, lax.div(b, 2))(lambda j: keys(j, False))
        keys(lax.div(b, 2), True)

        for g in range(2):
            out = mix[g, :HEAD, :] * (1 / mix[g, HEAD : HEAD + 1, :])
            for n in range(4):
                seen[:, (4 * g + n) * HEAD : (4 * g + n + 1) * HEAD] = out[:, n * HEAD : (n + 1) * HEAD].T.astype(BF)

        owner, e = (1 - s) * k + s * o, (1 - s) * o + s * k
        is_mine = 1 - lax.rem(owner + c, 2)
        into = is_mine * k + (1 - is_mine) * 2
        for t in range(4):
            acc[into, t] = dot(seen[...], dn[t // 3, pl.ds(t % 3 * 1024, 1024), :])

        @pl.when(owner != c)
        def _():
            @pl.loop(0, 4)
            def _(t):
                ds[s, e, t] = acc[2, t].astype(BF)
                pair(0, s, e, t).start()

    def combine_rows(o):
        @pl.loop(0, 4)
        def _(t):
            pair(0, 0, o, t).wait_recv()
            xs[o, t] = (acc[c, t] + dr[0, o, t].astype(F32)).astype(BF)
            pltpu.make_async_remote_copy(
                src_ref=xs.at[o, t], dst_ref=xr.at[c, t], send_sem=sum_sem.at[0, 0, o, t], recv_sem=sum_sem.at[1, 0, c, t],
                device_id=place.far(o), device_id_type=MESH,
            ).start()

    def combine(k, t):
        pair(1, 0, k, t).wait_recv()
        xs[k, t] = (acc[2, t] + dr[0, k, t].astype(F32)).astype(BF)
        over(1, k, t).start()

    @pl.loop(0, 4)
    def _(u):
        @pl.when(u == 1)
        def _():
            @pl.when(c == 0)
            def _():
                own[0][1].wait_recv()

            @pl.when(c == 1)
            def _():
                own[0][0].wait_recv()

        for k in range(2):

            @pl.when(u == 2 + k)
            def _(k=k):
                for n in range(2):
                    pass_on(0, k, n)
                received(handed[0][k])
                sent(hand[0][k])

        project(u)

        @pl.when(u == 2)
        def _():
            for w in loads_o:
                w.wait()

            @pl.loop(0, 2)
            def _(i):
                block(i)

            combine_rows(0)

    def gu_tile(j, slot):
        return [
            pltpu.make_async_copy(wg.at[:, at(j, PART)], gu.at[slot, :, 0:PART], gu_sem.at[slot, 0]),
            pltpu.make_async_copy(wu.at[:, at(j, PART)], gu.at[slot, :, PART : 2 * PART], gu_sem.at[slot, 1]),
        ]

    def gu_last(slot):
        cols, half = pl.ds(full * PART, PART // 2), PART // 2
        return [
            pltpu.make_async_copy(wg.at[:, cols], gu.at[slot, :, 0:half], gu_sem.at[slot, 0]),
            pltpu.make_async_copy(wu.at[:, cols], gu.at[slot, :, half:PART], gu_sem.at[slot, 1]),
        ]

    def d_tile(t):
        slot = lax.rem(t, D_SLOTS)
        rows = [pl.ds(i * units // D_PARTS, units // D_PARTS) for i in range(D_PARTS)]
        return [pltpu.make_async_copy(wd.at[r, at(t, WIDE)], dn.at[slot, r], d_sem.at[slot, i]) for i, r in enumerate(rows)]


    for j in range(GU_SLOTS):
        for w in gu_tile(j, j):
            w.start()
    for who in (place.partner, place.across):
        pl.semaphore_signal(free_sem, inc=1, device_id=who, device_id_type=MESH)
    for k in range(2):
        own[0][k].wait_send()
        sent(cross[0][k])

    def finish(f, k, t):
        pair(f, 1, k, t).wait_recv()
        over(f, k, t).wait_recv()
        rows, cols = at(k, HALF), at(t, WIDE)
        term = acc[k, t] + dr[1, k, t].astype(F32) + xr[k, t].astype(F32)
        res[rows, cols] = (res[rows, cols].astype(F32) + term).astype(BF)

    def own_half(k):
        @pl.loop(0, 4)
        def _(t):
            finish(0, k, t)

        norm_into(res, a.at[0], gain_m, k * HALF)
        own[1][k].start()

    @pl.loop(2, 8)
    def _(i):
        block(i)

        @pl.when(i == 3 + c)
        def _():
            combine_rows(1)

        @pl.when(i == 5)
        def _():
            pl.semaphore_wait(free_sem, 2)

        for k in range(2):

            @pl.when((c == 0) & (i == 5 + k))
            def _(k=k):
                own_half(k)

    def last_tile(lhs, into):
        r = dot(lhs[...], gu[full % GU_SLOTS, :, 0:PART])
        into[:, full * PART :] = (jax.nn.silu(r[:, : PART // 2]) * r[:, PART // 2 :]).astype(BF)

    @pl.loop(0, 4)
    def _(p):
        near, odd = 1 - lax.div(p, 2), lax.rem(p, 2)
        lhs = a.at[near * (c + p * (1 - 2 * c)) + (1 - near) * p]
        k = p - 2
        into = hid.at[near * p + (1 - near) * 2]

        @pl.when((p < 2) & (p != c))
        def _():
            own[1][0].wait_recv()
            own[1][1].wait_recv()

        @pl.when(p == 2)
        def _():
            received(hand[1][0])

        @pl.when(p == 3)
        def _():
            received(hand[1][1])

        @pl.when(odd == 1)
        def _():
            last_tile(lhs, into)
            begin(gu_tile(full - GU_SLOTS, full % GU_SLOTS))

        @pl.loop(0, full)
        def _(j):
            i = (1 - odd) * j + odd * (full - 1 - j)
            slot = lax.rem(i, GU_SLOTS)

            @pl.when((p == 0) | (j + odd >= GU_SLOTS))
            def _():
                await_(gu_tile(i, slot))

            r = dot(lhs[...], gu[slot])
            into[:, at(i, PART)] = (jax.nn.silu(r[:, :PART]) * r[:, PART:]).astype(BF)

            later = i + GU_SLOTS * (1 - 2 * odd)

            @pl.when((later >= 0) & (later < full))
            def _():
                begin(gu_tile(later, slot))

            @pl.when(p == 0)
            def _():
                @pl.when(j == full - 2)
                def _():
                    for t in range(D_SLOTS):
                        begin(d_tile(t))

                @pl.when((c == 0) & (j == 5))
                def _():
                    begin(cross[1][0])

                for k in range(2):

                    @pl.when((c == 1) & (j == 9 + k))
                    def _(k=k):
                        own_half(k)
                        begin(cross[1][k])

            @pl.when((odd == 0) & (later == full))
            def _():
                begin(gu_last(slot))

            @pl.when((odd == 1) & ((j == 1) | (j >= full - 3)))
            def _():
                @pl.when((p == 1) & (c == 0) & (j == full - 3))
                def _():
                    begin(cross[1][1])

                for n in range(2):

                    @pl.when((p == 1) & (j == full - 3 + 2 * n))
                    def _(n=n):
                        pass_on(1, 0, n)

                @pl.when((p == 3) & (j == 1))
                def _():
                    combine(0, 3)

        @pl.when(odd == 0)
        def _():
            await_(gu_last(full % GU_SLOTS))
            last_tile(lhs, into)

        @pl.when(p == 1)
        def _():
            @pl.loop(0, 8)
            def _(i):
                kk, t = lax.div(i, 4), lax.rem(i, 4)
                over(0, kk, t).wait_send()
                pair(0, 0, kk, t).wait_send()
                pair(0, 1, kk, t).wait_send()

        @pl.when(p >= 2)
        def _():
            @pl.loop(0, 4)
            def _(q):
                t = (1 - k) * q + k * (3 - q)

                @pl.when((k == 0) | (q >= D_SLOTS))
                def _():
                    await_(d_tile(t))

                r = dot(into[...], dn[lax.rem(t, D_SLOTS)])

                @pl.when((k == 0) & (q < 2))
                def _():
                    begin(d_tile(t + 2))

                @pl.when(k == 1)
                def _():
                    begin(d_tile(lax.rem(t + 2, 4)))

                acc[2, t] = r[:HALF]
                ds[0, k, t] = r[HALF:].astype(BF)
                pair(1, 0, k, t).start()

                @pl.when((q > 1) | ((q == 1) & (k == 0)))
                def _():
                    combine(k, t - 1 + 2 * k)

                @pl.when((q == 0) & (k == 1))
                def _():
                    combine(1, 3)

                @pl.when((p == 2) & (q == 1))
                def _():
                    for n in range(2):
                        pass_on(1, 1, n)

    def finish_tile(t):
        for k in range(2):
            finish(1, k, t)

    @pl.loop(0, 4)
    def _(q):
        t = 3 - q
        await_(d_tile(t))
        w = dn.at[lax.rem(t, D_SLOTS)]
        r = dot(hid[1 - c], w[...])
        for k in range(2):
            ds[1, k, t] = r[k * HALF : (k + 1) * HALF].astype(BF)
            pair(1, 1, k, t).start()

        @pl.when(q == 0)
        def _():
            combine(1, 0)

        r = dot(hid[c], w[...])
        for k in range(2):
            acc[k, t] = r[k * HALF : (k + 1) * HALF]

        @pl.when(q < 4 - D_SLOTS)
        def _():
            begin(d_tile(t - D_SLOTS))

        @pl.when(q > 0)
        def _():
            finish_tile(t + 1)

    finish_tile(0)

    @pl.loop(0, 8)
    def _(i):
        k, t = lax.div(i, 4), lax.rem(i, 4)
        over(1, k, t).wait_send()
        pair(1, 0, k, t).wait_send()
        pair(1, 1, k, t).wait_send()

    for k in range(2):
        own[1][k].wait_send()
        sent(cross[1][k])
        sent(hand[1][k])


def turns(rows):
    half = HEAD // 2
    rate = (float(THETA) ** (-np.arange(half, dtype=np.float32) / half)).astype(np.float32)
    angle = np.arange(rows, dtype=np.float32)[:, None] * rate
    cos, sin = np.cos(angle.astype(np.float64)), np.sin(angle.astype(np.float64))
    both = np.stack([np.concatenate([cos, cos], 1), np.concatenate([-sin, sin], 1)]).astype(np.float32)
    return both.reshape(2, rows // HALF, HALF, HEAD)


def solution(mesh):
    def step(x, gain_a, wq, wk, wv, wo, gain_m, w_gate, w_up, w_down):
        rows, d = x.shape
        units = w_gate.shape[1]
        dma = lambda *s: pltpu.SemaphoreType.DMA(s)
        tiles = (2, 4, HALF, WIDE)
        table = jnp.asarray(turns(4 * rows))
        anywhere, vmem = pl.BlockSpec(memory_space=pl.ANY), pl.BlockSpec(memory_space=pltpu.VMEM)
        return pl.pallas_call(
            layer,
            out_shape=pltpu.VMEM(x.shape, BF),
            in_specs=[anywhere, vmem, vmem] + [anywhere] * 8,
            out_specs=vmem,
            scratch_shapes=[
                pltpu.VMEM((4, rows, d), BF), pltpu.VMEM((GU_SLOTS, d, 2 * PART), BF),
                pltpu.VMEM((D_SLOTS, units, WIDE), BF), pltpu.VMEM(table.shape, F32), pltpu.VMEM((256, 512), BF),
                pltpu.VMEM((HALF, 1024), BF), pltpu.VMEM((2, 512), F32), pltpu.VMEM((2, HEAD + 16, 512), F32),
                pltpu.VMEM((3, *tiles[1:]), F32),
                pltpu.VMEM((2, *tiles), BF), pltpu.VMEM((2, *tiles), BF), pltpu.VMEM(tiles, BF), pltpu.VMEM(tiles, BF),
                pltpu.VMEM((3, rows, units), BF),
                dma(3), dma(4), dma(4), dma(GU_SLOTS, 2), dma(D_SLOTS, D_PARTS), dma(2, 2, 2), dma(2, 2, 2, 2), dma(2, 2, 2, 2), dma(2, 2, 2, 2, 4),
                dma(2, 2, 2, 4), pltpu.SemaphoreType.REGULAR,
            ],
            compiler_params=pltpu.CompilerParams(collective_id=0, has_side_effects=True, vmem_limit_bytes=VMEM_LIMIT),
            cost_estimate=pl.CostEstimate(flops=104_000_000_000, bytes_accessed=320_000_000, transcendentals=0),
            name="layer",
        )(x, gain_a, gain_m, table, wq, wk, wv, wo, w_gate, w_up, w_down)

    tokens, columns, rows_of = P(("dp", "tp"), None), P(None, "tp"), P("tp", None)
    return jax.shard_map(
        step,
        mesh=mesh,
        in_specs=(tokens, P(None), columns, columns, columns, rows_of, P(None), columns, columns, rows_of),
        out_specs=tokens,
        check_vma=False,
    )
```

```python
import jax
import jax.numpy as jnp
import numpy as np
from jax import lax
from jax.experimental import pallas as pl
from jax.experimental.pallas import tpu as pltpu
from jax.sharding import PartitionSpec as P

MESH = pl.DeviceIdType.MESH
BF, F32 = jnp.bfloat16, jnp.float32
HEAD = 128
THETA = 10000
NEG = -1e30
HIDDEN = 2 * NEG
E = HEAD**-0.5 * 1.4426950408889634
HALF = 128
PIECE = HALF // 2
WIDE = 1024
VMEM_LIMIT = 67043328 - 2**21


def dot(a, b):
    return jnp.dot(a, b, preferred_element_type=F32)


class Place:
    def __init__(self):
        tp, dp = lax.axis_index("tp"), lax.axis_index("dp")
        self.c, self.x, self.dp = lax.rem(tp, 2), lax.div(tp, 2), dp
        self.partner = (dp, self.x * 2 + (1 - self.c))
        self.across = (dp, (1 - self.x) * 2 + self.c)

    def greet(self):
        barrier = pltpu.get_barrier_semaphore()
        for who in (self.partner, self.across, self.far(1 - self.c)):
            pl.semaphore_signal(barrier, inc=1, device_id=who, device_id_type=MESH)
        pl.semaphore_wait(barrier, 3)

    def far(self, core):
        return self.dp, (1 - self.x) * 2 + core


def remote(src, dst, sems, at, who):
    return pltpu.make_async_remote_copy(
        src_ref=src, dst_ref=dst, send_sem=sems.at[(0, *at)], recv_sem=sems.at[(1, *at)], device_id=who, device_id_type=MESH
    )


def norm_into(src, dst, gain, first, count=HALF):
    @pl.loop(0, count // 32)
    def _(i):
        rows = pl.ds(pl.multiple_of(first + i * 32, 32), 32)
        wide = src[rows, :].astype(F32)
        scale = lax.rsqrt(jnp.mean(wide * wide, -1, keepdims=True) + 1e-6)
        dst[rows, :] = (wide * scale * gain[...].astype(F32)).astype(BF)


PART = 256
GU_SLOTS, D_SLOTS = 3, 2
D_PARTS = 4


def at(i, size):
    return pl.ds(pl.multiple_of(i * size, size), size)


def layer(x_hbm, gain_a, gain_m, tab_hbm, wq, wk, wv, wo, wg, wu, wd, res, a, gu, dn, tab, tq, seen, top, mix, acc,
          ds, dr, xs, xr, hid, load_sem, w_sem, wo_sem, gu_sem, d_sem, own_sem, cross_sem, hand_sem, pair_sem, sum_sem, free_sem):
    place = Place()
    c, x = place.c, place.x
    units = wg.shape[1]
    full = units // PART
    tiles = full + 1
    halves = [pl.ds(k * HALF, HALF) for k in range(2)]
    load = [pltpu.make_async_copy(x_hbm.at[r], res.at[r], load_sem.at[k]) for k, r in enumerate(halves)]
    for w in load:
        w.start()
    load_tab = pltpu.make_async_copy(tab_hbm, tab, load_sem.at[2])
    loads = [
        pltpu.make_async_copy(wq.at[:, 0:512], gu.at[0], w_sem.at[0]),
        pltpu.make_async_copy(wq.at[:, 512:1024], gu.at[1], w_sem.at[1]),
        pltpu.make_async_copy(wk, gu.at[2, :, 0:256], w_sem.at[2]),
        pltpu.make_async_copy(wv, gu.at[2, :, 256:512], w_sem.at[3]),
    ]
    loads_o = [
        pltpu.make_async_copy(wo.at[:, t * WIDE : (t + 1) * WIDE], dn.at[t // 3, pl.ds(t % 3 * 1024, 1024)], wo_sem.at[t]) for t in range(4)
    ]

    def pieces(half):
        return [pl.ds(pl.multiple_of(half * HALF + n * PIECE, PIECE), PIECE) for n in range(2)]

    def copies(src, dst, src_half, dst_half, sems, f, k, who):
        rows = zip(pieces(src_half), pieces(dst_half), strict=True)
        return [remote(a.at[src, r], a.at[dst, q], sems, (f, k, n), who) for n, (r, q) in enumerate(rows)]

    own = [[remote(a.at[0, r], a.at[1, r], own_sem, (f, k), place.partner) for k, r in enumerate(halves)] for f in range(2)]
    cross = [
        [copies(lax.rem(c + k, 2), 2 + k, c, c, cross_sem, 0, k, place.across) for k in range(2)],
        [copies(0, 2 + k, k, 0, cross_sem, 1, k, place.across) for k in range(2)],
    ]
    hand = [
        [copies(2 + k, 2 + k, c, c, hand_sem, 0, k, place.partner) for k in range(2)],
        [copies(2 + k, 2 + k, 0, 1, hand_sem, 1, k, place.partner) for k in range(2)],
    ]
    handed = [[copies(2 + k, 2 + k, 1 - c, 1 - c, hand_sem, 0, k, place.partner) for k in range(2)], hand[1]]

    def pass_on(f, k, n):
        cross[f][k][n].wait_recv()
        hand[f][k][n].start()

    def begin(copies):
        for w in copies:
            w.start()

    def received(copies):
        for w in copies:
            w.wait_recv()

    def sent(copies):
        for w in copies:
            w.wait_send()

    def await_(copies):
        for w in copies:
            w.wait()

    def pair(f, s, k, t):
        return remote(ds.at[s, k, t], dr.at[s, k, t], pair_sem, (f, s, k, t), place.partner)

    def over(f, k, t):
        return remote(xs.at[k, t], xr.at[k, t], sum_sem, (f, k, t), place.across)

    place.greet()
    load[0].wait()
    for n in range(2):
        norm_into(res, a.at[0], gain_a, n * PIECE, PIECE)

        @pl.when(c == 0)
        def _(n=n):
            cross[0][0][n].start()

    own[0][0].start()

    load[1].wait()
    for w in (*loads, load_tab, *loads_o):
        w.start()
    norm_into(res, a.at[0], gain_a, HALF)
    own[0][1].start()
    hid[2] = jnp.zeros(hid.shape[1:], BF)
    hid[2, HEAD : HEAD + 16, 1024:3072] = jnp.ones((16, 2048), BF)

    @pl.when(c == 0)
    def _():
        own[0][0].wait_recv()
        begin(cross[0][1])

    @pl.when(c == 1)
    def _():
        own[0][1].wait_recv()
        begin(cross[0][0])
        begin(cross[0][1])

    load_tab.wait()
    for w in loads:
        w.wait()

    def queries(b):
        return lax.div(b, 6), at(lax.rem(b, 2), HALF), lax.div(lax.rem(b, 6), 2) * 8

    def project(u):
        far = lax.div(u, 2)
        core = c + u * (1 - 2 * c)
        b0 = (1 - far) * (x * 4 + core * 2) + far * ((1 - x) * 4 + (u - 2) * 2)

        @pl.loop(0, 3)
        def _(j):
            tq[...] = dot(a[u], gu[j]).astype(BF)
            for half in range(2):
                b = b0 + half

                def part(n, half=half):
                    return tq[half * HALF : (half + 1) * HALF, n * HEAD : (n + 1) * HEAD]

                def turned(n, b=b, part=part):
                    t = part(n).astype(F32)
                    return (t * tab[0, b] + pltpu.roll(t, HEAD // 2, 1) * tab[1, b]).astype(BF)

                @pl.when(j < 2)
                def _():
                    slot, rows, first = queries(b)
                    for n in range(4):
                        hid[slot, rows, at(first + j * 4 + n, HEAD)] = turned(n)

                @pl.when(j == 2)
                def _():
                    for n in range(2):
                        hid[2, at(lax.rem(b, 2), HALF), at(n * 4 + lax.div(b, 2), HEAD)] = turned(n)
                        hid[2, :HEAD, at(8 + n * 8 + b, HALF)] = part(2 + n).T

    def block(i):
        s, o, k = lax.div(i, 4), lax.div(lax.rem(i, 4), 2), lax.rem(i, 2)
        b = ((1 - s) * (1 - x) + s * x) * 4 + lax.rem(i, 4)
        top[...] = jnp.full_like(top, NEG)
        mix[...] = jnp.zeros_like(mix)
        slot, rows, first = queries(b)

        def query(g):
            return jnp.concatenate([hid[slot, rows, at(first + 4 * g + n, HEAD)] for n in range(4)], axis=0)

        def keys(j, masked):
            if masked:
                gap = lax.rem(lax.broadcasted_iota(jnp.int32, (256, 512), 1), HALF) - lax.broadcasted_iota(jnp.int32, (256, 512), 0)
                ok = gap >= j * 256 - b * HALF
            scores = [
                lax.dot_general(hid[2, :, at(g * 4 + j, HEAD)], query(g), (((1,), (1,)), ((), ())), preferred_element_type=F32)
                for g in range(2)
            ]
            weights, keeps = [], []
            for g in range(2):
                sc = jnp.where(ok, scores[g], HIDDEN) if masked else scores[g]
                old = top[g : g + 1, :]
                new = jnp.maximum(old, sc.max(axis=0, keepdims=True))
                top[g : g + 1, :] = new
                weights.append(jnp.exp2((sc - new) * E).astype(BF))
                keeps.append(jnp.exp2((old - new) * E))
            for g in range(2):
                mix[g] = mix[g] * keeps[g] + dot(hid[2, : HEAD + 16, at(4 + g * 4 + j, 256)], weights[g])

        pl.loop(0, lax.div(b, 2))(lambda j: keys(j, False))
        keys(lax.div(b, 2), True)

        for g in range(2):
            out = mix[g, :HEAD, :] * (1 / mix[g, HEAD : HEAD + 1, :])
            for n in range(4):
                seen[:, (4 * g + n) * HEAD : (4 * g + n + 1) * HEAD] = out[:, n * HEAD : (n + 1) * HEAD].T.astype(BF)

        owner, e = (1 - s) * k + s * o, (1 - s) * o + s * k
        is_mine = 1 - lax.rem(owner + c, 2)
        into = is_mine * k + (1 - is_mine) * 2
        for t in range(4):
            acc[into, t] = dot(seen[...], dn[t // 3, pl.ds(t % 3 * 1024, 1024), :])

        @pl.when(owner != c)
        def _():
            @pl.loop(0, 4)
            def _(t):
                ds[s, e, t] = acc[2, t].astype(BF)
                pair(0, s, e, t).start()

    def combine_rows(o):
        @pl.loop(0, 4)
        def _(t):
            pair(0, 0, o, t).wait_recv()
            xs[o, t] = (acc[c, t] + dr[0, o, t].astype(F32)).astype(BF)
            pltpu.make_async_remote_copy(
                src_ref=xs.at[o, t], dst_ref=xr.at[c, t], send_sem=sum_sem.at[0, 0, o, t], recv_sem=sum_sem.at[1, 0, c, t],
                device_id=place.far(o), device_id_type=MESH,
            ).start()

    def combine(k, t):
        pair(1, 0, k, t).wait_recv()
        xs[k, t] = (acc[2, t] + dr[0, k, t].astype(F32)).astype(BF)
        over(1, k, t).start()

    @pl.loop(0, 4)
    def _(u):
        @pl.when(u == 1)
        def _():
            @pl.when(c == 0)
            def _():
                own[0][1].wait_recv()

            @pl.when(c == 1)
            def _():
                own[0][0].wait_recv()

        for k in range(2):

            @pl.when(u == 2 + k)
            def _(k=k):
                for n in range(2):
                    pass_on(0, k, n)
                received(handed[0][k])
                sent(hand[0][k])

        project(u)

        @pl.when(u == 2)
        def _():
            for w in loads_o:
                w.wait()

            @pl.loop(0, 2)
            def _(i):
                block(i)

            combine_rows(0)

    def gu_tile(j, slot):
        return [
            pltpu.make_async_copy(wg.at[:, at(j, PART)], gu.at[slot, :, 0:PART], gu_sem.at[slot, 0]),
            pltpu.make_async_copy(wu.at[:, at(j, PART)], gu.at[slot, :, PART : 2 * PART], gu_sem.at[slot, 1]),
        ]

    def gu_last(slot):
        cols, half = pl.ds(full * PART, PART // 2), PART // 2
        return [
            pltpu.make_async_copy(wg.at[:, cols], gu.at[slot, :, 0:half], gu_sem.at[slot, 0]),
            pltpu.make_async_copy(wu.at[:, cols], gu.at[slot, :, half:PART], gu_sem.at[slot, 1]),
        ]

    def d_tile(t):
        slot = lax.rem(t, D_SLOTS)
        rows = [pl.ds(i * units // D_PARTS, units // D_PARTS) for i in range(D_PARTS)]
        return [pltpu.make_async_copy(wd.at[r, at(t, WIDE)], dn.at[slot, r], d_sem.at[slot, i]) for i, r in enumerate(rows)]


    for j in range(GU_SLOTS):
        for w in gu_tile(j, j):
            w.start()
    for who in (place.partner, place.across):
        pl.semaphore_signal(free_sem, inc=1, device_id=who, device_id_type=MESH)
    for k in range(2):
        own[0][k].wait_send()
        sent(cross[0][k])

    def finish(f, k, t):
        pair(f, 1, k, t).wait_recv()
        over(f, k, t).wait_recv()
        rows, cols = at(k, HALF), at(t, WIDE)
        term = acc[k, t] + dr[1, k, t].astype(F32) + xr[k, t].astype(F32)
        res[rows, cols] = (res[rows, cols].astype(F32) + term).astype(BF)

    def own_half(k):
        @pl.loop(0, 4)
        def _(t):
            finish(0, k, t)

        norm_into(res, a.at[0], gain_m, k * HALF)
        own[1][k].start()

    @pl.loop(2, 8)
    def _(i):
        block(i)

        @pl.when(i == 3 + c)
        def _():
            combine_rows(1)

        @pl.when(i == 5)
        def _():
            pl.semaphore_wait(free_sem, 2)

        for k in range(2):

            @pl.when((c == 0) & (i == 5 + k))
            def _(k=k):
                own_half(k)

    def last_tile(lhs, into):
        r = dot(lhs[...], gu[full % GU_SLOTS, :, 0:PART])
        into[:, full * PART :] = (jax.nn.silu(r[:, : PART // 2]) * r[:, PART // 2 :]).astype(BF)

    @pl.loop(0, 4)
    def _(p):
        near, odd = 1 - lax.div(p, 2), lax.rem(p, 2)
        lhs = a.at[near * (c + p * (1 - 2 * c)) + (1 - near) * p]
        k = p - 2
        into = hid.at[near * p + (1 - near) * 2]

        @pl.when((p < 2) & (p != c))
        def _():
            own[1][0].wait_recv()
            own[1][1].wait_recv()

        @pl.when(p == 2)
        def _():
            received(hand[1][0])

        @pl.when(p == 3)
        def _():
            received(hand[1][1])

        @pl.when(odd == 1)
        def _():
            last_tile(lhs, into)
            begin(gu_tile(full - GU_SLOTS, full % GU_SLOTS))

        @pl.loop(0, full)
        def _(j):
            i = (1 - odd) * j + odd * (full - 1 - j)
            slot = lax.rem(i, GU_SLOTS)

            @pl.when((p == 0) | (j + odd >= GU_SLOTS))
            def _():
                await_(gu_tile(i, slot))

            r = dot(lhs[...], gu[slot])
            into[:, at(i, PART)] = (jax.nn.silu(r[:, :PART]) * r[:, PART:]).astype(BF)

            later = i + GU_SLOTS * (1 - 2 * odd)

            @pl.when((later >= 0) & (later < full))
            def _():
                begin(gu_tile(later, slot))

            @pl.when(p == 0)
            def _():
                @pl.when(j == full - 2)
                def _():
                    for t in range(D_SLOTS):
                        begin(d_tile(t))

                @pl.when((c == 0) & (j == 3))
                def _():
                    begin(cross[1][0])

                for k in range(2):

                    @pl.when((c == 1) & (j == 8 + 2 * k))
                    def _(k=k):
                        own_half(k)
                        begin(cross[1][k])

            @pl.when((odd == 0) & (later == full))
            def _():
                begin(gu_last(slot))

            @pl.when((odd == 1) & ((j == 1) | (j >= full - 3)))
            def _():
                @pl.when((p == 1) & (c == 0) & (j == full - 3))
                def _():
                    begin(cross[1][1])

                for n in range(2):

                    @pl.when((p == 1) & (j == full - 3 + 2 * n))
                    def _(n=n):
                        pass_on(1, 0, n)

                @pl.when((p == 3) & (j == 1))
                def _():
                    combine(0, 3)

        @pl.when(odd == 0)
        def _():
            await_(gu_last(full % GU_SLOTS))
            last_tile(lhs, into)

        @pl.when(p == 1)
        def _():
            @pl.loop(0, 8)
            def _(i):
                kk, t = lax.div(i, 4), lax.rem(i, 4)
                over(0, kk, t).wait_send()
                pair(0, 0, kk, t).wait_send()
                pair(0, 1, kk, t).wait_send()

        @pl.when(p >= 2)
        def _():
            @pl.loop(0, 4)
            def _(q):
                t = (1 - k) * q + k * (3 - q)

                @pl.when((k == 0) | (q >= D_SLOTS))
                def _():
                    await_(d_tile(t))

                r = dot(into[...], dn[lax.rem(t, D_SLOTS)])

                @pl.when((k == 0) & (q < 2))
                def _():
                    begin(d_tile(t + 2))

                @pl.when(k == 1)
                def _():
                    begin(d_tile(lax.rem(t + 2, 4)))

                acc[2, t] = r[:HALF]
                ds[0, k, t] = r[HALF:].astype(BF)
                pair(1, 0, k, t).start()

                @pl.when((q > 1) | ((q == 1) & (k == 0)))
                def _():
                    combine(k, t - 1 + 2 * k)

                @pl.when((q == 0) & (k == 1))
                def _():
                    combine(1, 3)

                @pl.when((p == 2) & (q == 1))
                def _():
                    for n in range(2):
                        pass_on(1, 1, n)

    def finish_tile(t):
        for k in range(2):
            finish(1, k, t)

    @pl.loop(0, 4)
    def _(q):
        t = 3 - q
        await_(d_tile(t))
        w = dn.at[lax.rem(t, D_SLOTS)]
        r = dot(hid[1 - c], w[...])
        for k in range(2):
            ds[1, k, t] = r[k * HALF : (k + 1) * HALF].astype(BF)
            pair(1, 1, k, t).start()

        @pl.when(q == 0)
        def _():
            combine(1, 0)

        r = dot(hid[c], w[...])
        for k in range(2):
            acc[k, t] = r[k * HALF : (k + 1) * HALF]

        @pl.when(q < 4 - D_SLOTS)
        def _():
            begin(d_tile(t - D_SLOTS))

        @pl.when(q > 0)
        def _():
            finish_tile(t + 1)

    finish_tile(0)

    @pl.loop(0, 8)
    def _(i):
        k, t = lax.div(i, 4), lax.rem(i, 4)
        over(1, k, t).wait_send()
        pair(1, 0, k, t).wait_send()
        pair(1, 1, k, t).wait_send()

    for k in range(2):
        own[1][k].wait_send()
        sent(cross[1][k])
        sent(hand[1][k])


def turns(rows):
    half = HEAD // 2
    rate = (float(THETA) ** (-np.arange(half, dtype=np.float32) / half)).astype(np.float32)
    angle = np.arange(rows, dtype=np.float32)[:, None] * rate
    cos, sin = np.cos(angle.astype(np.float64)), np.sin(angle.astype(np.float64))
    both = np.stack([np.concatenate([cos, cos], 1), np.concatenate([-sin, sin], 1)]).astype(np.float32)
    return both.reshape(2, rows // HALF, HALF, HEAD)


def solution(mesh):
    def step(x, gain_a, wq, wk, wv, wo, gain_m, w_gate, w_up, w_down):
        rows, d = x.shape
        units = w_gate.shape[1]
        dma = lambda *s: pltpu.SemaphoreType.DMA(s)
        tiles = (2, 4, HALF, WIDE)
        table = jnp.asarray(turns(4 * rows))
        anywhere, vmem = pl.BlockSpec(memory_space=pl.ANY), pl.BlockSpec(memory_space=pltpu.VMEM)
        return pl.pallas_call(
            layer,
            out_shape=pltpu.VMEM(x.shape, BF),
            in_specs=[anywhere, vmem, vmem] + [anywhere] * 8,
            out_specs=vmem,
            scratch_shapes=[
                pltpu.VMEM((4, rows, d), BF), pltpu.VMEM((GU_SLOTS, d, 2 * PART), BF),
                pltpu.VMEM((D_SLOTS, units, WIDE), BF), pltpu.VMEM(table.shape, F32), pltpu.VMEM((256, 512), BF),
                pltpu.VMEM((HALF, 1024), BF), pltpu.VMEM((2, 512), F32), pltpu.VMEM((2, HEAD + 16, 512), F32),
                pltpu.VMEM((3, *tiles[1:]), F32),
                pltpu.VMEM((2, *tiles), BF), pltpu.VMEM((2, *tiles), BF), pltpu.VMEM(tiles, BF), pltpu.VMEM(tiles, BF),
                pltpu.VMEM((3, rows, units), BF),
                dma(3), dma(4), dma(4), dma(GU_SLOTS, 2), dma(D_SLOTS, D_PARTS), dma(2, 2, 2), dma(2, 2, 2, 2), dma(2, 2, 2, 2), dma(2, 2, 2, 2, 4),
                dma(2, 2, 2, 4), pltpu.SemaphoreType.REGULAR,
            ],
            compiler_params=pltpu.CompilerParams(collective_id=0, has_side_effects=True, vmem_limit_bytes=VMEM_LIMIT),
            cost_estimate=pl.CostEstimate(flops=104_000_000_000, bytes_accessed=320_000_000, transcendentals=0),
            name="layer",
        )(x, gain_a, gain_m, table, wq, wk, wv, wo, w_gate, w_up, w_down)

    tokens, columns, rows_of = P(("dp", "tp"), None), P(None, "tp"), P("tp", None)
    return jax.shard_map(
        step,
        mesh=mesh,
        in_specs=(tokens, P(None), columns, columns, columns, rows_of, P(None), columns, columns, rows_of),
        out_specs=tokens,
        check_vma=False,
    )
```
